128 devices in a mesh: rows: 4 (over y_lo, core), cols: 32 (over z, y_hi, x).
Axes of the slice: x: 4, y: 4 (y_hi: 2, y_lo: 2; y = y_hi * 2 + y_lo), z: 4, core: 2. Of those that a mesh axis runs over, the one named last changes fastest.
Arguments:
- tracer: float32 [384, 1024, 128], P('rows', 'cols'), may hold values from 0.2 to 1.8
- crowding: float32 [384, 1024, 128], P('rows', 'cols'), may hold values from 0.5 to 2
Outputs:
- potential: float32 [384, 1024, 128], P('rows', 'cols')
- tracer_end: float32 [384, 1024, 128], P('rows', 'cols')
The draws below stay inside these ranges and needn't reach their ends.
All inputs are finite; a program needn't handle non-finite values.
Results may differ from the reference program's by a relative error of at most 0.00002.
Values sent between devices are 32-bit elements; how exact they have to be, the bound alone decides.
A program may use at most 64 MiB of HBM per device.

```python
import jax
import jax.numpy as jnp
from jax import lax

GRID_Y = 384
GRID_X = 1024
MEMBERS = 128
STEPS = 6


def block_levels(stream_key, extent, pieces, smallest, largest):
    def one(dim, parts):
        draws = jax.random.uniform(jax.random.fold_in(jax.random.fold_in(stream_key, 6), dim), (parts,), jnp.float32, smallest / len(pieces), largest / len(pieces))
        return jnp.repeat(jnp.exp(draws), extent[dim] // parts).reshape((-1,) + (1,) * (len(extent) - dim - 1))

    loudness = one(*pieces[0])
    for cut in pieces[1:]:
        loudness = loudness * one(*cut)
    return loudness


def setup_inputs(seed: int = 0) -> dict:
    streams_of = jax.random.split(jax.random.key(seed), 3)
    tracer = jnp.clip(0.2 + 1.5999999 * jax.random.uniform(streams_of[0], (GRID_Y, GRID_X, MEMBERS), jnp.float32) ** block_levels(streams_of[0], (GRID_Y, GRID_X, MEMBERS), ((0, 4), (1, 32)), -0.2, 0.2), 0.2, 1.8)
    crowding = jnp.clip(0.5 + 1.5 * jax.random.uniform(streams_of[1], (GRID_Y, GRID_X, MEMBERS), jnp.float32) ** block_levels(streams_of[1], (GRID_Y, GRID_X, MEMBERS), ((0, 4), (1, 32)), -0.2, 0.2), 0.5, 2.0)
    return dict(tracer=tracer, crowding=crowding)


def strip_edges(values, dims):
    for dim in dims:
        values = lax.slice_in_dim(values, 1, values.shape[dim] - 1, axis=dim)
    return values


def neighbour(values, dim, start, dims):
    others = [other for other in dims if other != dim]
    values = strip_edges(values, others)
    return lax.slice_in_dim(values, start, start + values.shape[dim] - 2, axis=dim)


def one_step(padded, crowding):
    middle = strip_edges(padded, (0, 1))
    lower = [neighbour(padded, dim, 0, (0, 1)) for dim in (0, 1)]
    upper = [neighbour(padded, dim, 2, (0, 1)) for dim in (0, 1)]
    spread = lower[0] + upper[0] + lower[1] + upper[1] - 4.0 * middle
    return middle + 0.1 * spread + 0.2 * middle * (1.0 - middle * crowding)


def reference(tracer, crowding):
    for step in range(STEPS):
        tracer = one_step(jnp.pad(tracer, ((1, 1), (1, 1), (0, 0)), mode="constant"), crowding)
    potential = jnp.cumsum(tracer, axis=1) / GRID_X
    return potential, tracer
```

```python
import jax
import jax.numpy as jnp
from jax import lax
from jax.experimental import pallas as pl
from jax.experimental.pallas import tpu as pltpu
from jax.sharding import PartitionSpec as P

NY, NX, M = 96, 32, 128
PITCH = 40
Y0 = 8
ROWS = NY + 2 * Y0
DY, DX = 6, 3
QUARTER = NY // 4
MESH = pl.DeviceIdType.MESH
DIRECTIONS = [(dr, dc) for dr in (-1, 0, 1) for dc in (-1, 0, 1) if (dr, dc) != (0, 0)]


def rows_of(dr, depth):
    if dr == 0:
        return (0, NY), (0, NY)
    if dr < 0:
        return (0, depth), (NY, NY + depth)
    return (NY - depth, NY), (-depth, 0)


def window(ref, rows, side, depth):
    low, high = rows
    if side == "all":
        return ref.at[Y0 + low : Y0 + high, 0:NX, :]
    if side == "first":
        return ref.at[Y0 + low : Y0 + high, 0:depth, :]
    if side == "last":
        return ref.at[Y0 + low : Y0 + high, NX - depth : NX, :]
    if side == "right halo":
        return ref.at[Y0 + low : Y0 + high, NX : NX + depth, :]
    return ref.at[Y0 + low - 1 : Y0 + high - 1, PITCH - depth : PITCH, :]


def sides_of(dc):
    if dc == 0:
        return "all", "all"
    if dc < 0:
        return "first", "right halo"
    return "last", "left halo"


def kernel(
    tracer, crowding, end, here, below,
    u, v, w, t3, tot, p1, p2, group, back,
    in_sem, send_t, recv_t, send_w, recv_w, send_x, recv_x,
    send_1, recv_1, send_2, recv_2, send_3, recv_3,
):
    r = lax.axis_index("rows")
    c = lax.axis_index("cols")
    n_r, n_c = 4, 32
    x = lax.rem(c, 4)
    g = lax.div(c, 4)
    load_t = pltpu.make_async_copy(tracer, window(u, (0, NY), "all", 0), in_sem.at[0])
    load_w = pltpu.make_async_copy(crowding, window(w, (0, NY), "all", 0), in_sem.at[1])
    load_t.start()
    load_w.start()

    def exists(dr, dc):
        ok = True
        if dr < 0:
            ok = r > 0
        if dr > 0:
            ok = r < n_r - 1
        if dc < 0:
            ok = ok & (c > 0)
        if dc > 0:
            ok = ok & (c < n_c - 1)
        return ok

    def neighbour(dr, dc):
        return {"rows": r + dr, "cols": c + dc}

    barrier = pltpu.get_barrier_semaphore()
    group_peers = [{"cols": g * 4 + lax.rem(x + o, 4)} for o in (1, 2, 3)]
    line_peers = [{"cols": lax.rem(g + o, 8) * 4 + x} for o in range(1, 8)]
    expected = jnp.int32(len(group_peers) + len(line_peers))
    for peer in group_peers + line_peers:
        pl.semaphore_signal(barrier, inc=1, device_id=peer, device_id_type=MESH)
    for d in DIRECTIONS:
        here_too = exists(*d)
        expected = expected + here_too.astype(jnp.int32)

        @pl.when(here_too)
        def _(d=d):
            pl.semaphore_signal(barrier, inc=1, device_id=neighbour(*d), device_id_type=MESH)

    is_left, is_right, is_top, is_bottom = c == 0, c == n_c - 1, r == 0, r == n_r - 1
    flat = lambda ref: ref.reshape(ROWS * PITCH, M)

    def zero_sides(ref):
        f = flat(ref)
        zero = jnp.zeros((NY + 2 * DY, M), jnp.float32)

        @pl.when(is_left)
        def _():
            f[pl.ds((Y0 - DY) * PITCH - 1, NY + 2 * DY, stride=PITCH), :] = zero

        @pl.when(is_right)
        def _():
            f[pl.ds((Y0 - DY) * PITCH + NX, NY + 2 * DY, stride=PITCH), :] = zero

    def zero_rows(ref, halo):
        f = flat(ref)
        before, width = (4, PITCH) if halo else (0, NX)
        zero = jnp.zeros((width, M), jnp.float32)

        @pl.when(is_top)
        def _():
            f[pl.ds((Y0 - 1) * PITCH - before, width), :] = zero

        @pl.when(is_bottom)
        def _():
            f[pl.ds((Y0 + NY) * PITCH - before, width), :] = zero

    zero_sides(u)
    zero_sides(t3)

    @pl.when(is_top)
    def _():
        u[Y0 - 1, 0:NX, :] = jnp.zeros((NX, M), jnp.float32)

    @pl.when(is_bottom)
    def _():
        u[Y0 + NY, 0:NX, :] = jnp.zeros((NX, M), jnp.float32)

    load_t.wait()
    load_w.wait()
    pl.semaphore_wait(barrier, expected)

    def halo_copies(ref, dy, dx, send, recv, directions):
        out = []
        for k, (dr, dc) in enumerate(directions):
            source, target = rows_of(dr, dy)
            here_side, there_side = sides_of(dc)
            out.append(
                pltpu.make_async_remote_copy(
                    src_ref=window(ref, source, here_side, dx),
                    dst_ref=window(ref, target, there_side, dx),
                    send_sem=send.at[k],
                    recv_sem=recv.at[k],
                    device_id=neighbour(dr, dc),
                    device_id_type=MESH,
                )
            )
        return out

    copies_t = halo_copies(u, DY, DX, send_t, recv_t, DIRECTIONS)
    copies_w = halo_copies(w, DY - 1, DX - 1, send_w, recv_w, DIRECTIONS)
    for copies in (copies_t, copies_w):
        for d, copy in zip(DIRECTIONS, copies):
            pl.when(exists(*d))(copy.start)
    for copies in (copies_t, copies_w):
        for d, copy in zip(DIRECTIONS, copies):
            pl.when(exists(-d[0], -d[1]))(copy.wait_recv)

    fu, fv, fw, f3 = flat(u), flat(v), flat(w), flat(t3)

    def zero_rows_after_arrival(ref):
        zero_rows(ref, True)

    zero_rows_after_arrival(u)

    def step(src, low, high, tiles, store, first=False, last=False):
        def body(i, carry):
            north, centre = carry
            base = pl.multiple_of((Y0 + low + i) * PITCH, 8)
            south, new = [], []
            for k in range(tiles):
                at = base + 8 * k
                s = src[pl.ds(pl.multiple_of(at + PITCH, 8), 8), :]
                left = src[pl.ds(at - 1, 8), :]
                right = src[pl.ds(at + 1, 8), :]
                cr = fw[pl.ds(pl.multiple_of(at, 8), 8), :]
                here_ = centre[k]
                spread = (left + right) + (north[k] + s)
                used = here_ * cr
                if first:
                    used = used + used
                grown = spread + here_ * (8.0 - used)
                new.append(grown * (0.2 if first else 0.05 if last else 0.1))
                south.append(s)
            store(i, base, new)
            return tuple(centre), tuple(south)

        start = (Y0 + low - 1) * PITCH
        north = tuple(src[pl.ds(start + 8 * k, 8), :] for k in range(tiles))
        centre = tuple(src[pl.ds(start + PITCH + 8 * k, 8), :] for k in range(tiles))
        lax.fori_loop(0, high - low, body, (north, centre), unroll=2)

    def store_to(dst):
        def store(i, base, new):
            for k, value in enumerate(new):
                dst[pl.ds(pl.multiple_of(base + 8 * k, 8), 8), :] = value

        return store

    step(fu, -5, NY + 5, 5, store_to(fv), first=True)
    zero_sides(v)
    zero_rows(v, True)
    for d, copy in zip(DIRECTIONS, copies_t):
        pl.when(exists(*d))(copy.wait_send)
    step(fv, -4, NY + 4, 5, store_to(fu))
    zero_sides(u)
    zero_rows(u, True)
    step(fu, -3, NY + 3, 4, store_to(f3))
    zero_rows(t3, False)

    across = [(0, -1), (0, 1)]
    copies_x = []
    for k, (dr, dc) in enumerate(across):
        here_side, there_side = sides_of(dc)
        rows = (-DX, NY + DX)
        copies_x.append(
            pltpu.make_async_remote_copy(
                src_ref=window(t3, rows, here_side, DX),
                dst_ref=window(t3, rows, there_side, DX),
                send_sem=send_x.at[k],
                recv_sem=recv_x.at[k],
                device_id=neighbour(dr, dc),
                device_id_type=MESH,
            )
        )
    for d, copy in zip(across, copies_x):
        pl.when(exists(*d))(copy.start)
    for d, copy in zip(across, copies_x):
        pl.when(exists(-d[0], -d[1]))(copy.wait_recv)

    step(f3, -2, NY + 2, 5, store_to(fv))
    zero_sides(v)
    zero_rows(v, True)
    step(fv, -1, NY + 1, 5, store_to(fu))
    zero_sides(u)
    zero_rows(u, True)

    def store_end(i, base, new):
        for k, value in enumerate(new):
            end[i, 8 * k : 8 * k + 8, :] = value
        total = (new[0] + new[1]) + (new[2] + new[3])
        tot[pl.ds(i, 1), :] = jnp.sum(total, axis=0, keepdims=True)

    step(fu, 0, NY, 4, store_end, last=True)

    copies_1 = []
    for k, (o, peer) in enumerate(zip((1, 2, 3), group_peers)):
        to = lax.rem(x + o, 4)
        copies_1.append(
            pltpu.make_async_remote_copy(
                src_ref=tot.at[pl.ds(pl.multiple_of(to * QUARTER, 8), QUARTER), :],
                dst_ref=p1.at[x],
                send_sem=send_1.at[k],
                recv_sem=recv_1.at[k],
                device_id=peer,
                device_id_type=MESH,
            )
        )
    for copy in copies_1:
        copy.start()
    p1[x] = tot[pl.ds(pl.multiple_of(x * QUARTER, 8), QUARTER), :]

    place = lax.broadcasted_iota(jnp.int32, (8, M), 0)

    def running(i, _):
        carry = jnp.zeros((1, M), jnp.float32)
        for k in range(4):
            value = end[i, 8 * k : 8 * k + 8, :]
            for shift in (1, 2, 4):
                value = value + jnp.where(place >= shift, pltpu.roll(value, shift, 0), 0.0)
            value = value + carry
            here[i, 8 * k : 8 * k + 8, :] = value
            carry = value[7:8, :]
        return 0

    lax.fori_loop(0, NY, running, 0, unroll=2)

    for copy in copies_1:
        copy.wait_recv()
    own = [p1[k] for k in range(4)]
    group[...] = (own[0] + own[1]) + (own[2] + own[3])
    copies_2 = []
    for k, peer in enumerate(line_peers):
        copies_2.append(
            pltpu.make_async_remote_copy(
                src_ref=group,
                dst_ref=p2.at[g],
                send_sem=send_2.at[k],
                recv_sem=recv_2.at[k],
                device_id=peer,
                device_id_type=MESH,
            )
        )
    for copy in copies_2:
        copy.start()
    for copy in copies_2:
        copy.wait_recv()
    before = jnp.zeros((QUARTER, M), jnp.float32)
    for k in range(7):
        before = before + jnp.where(k < g, p2[k], 0.0)
    for k in range(4):
        back[k] = before
        before = before + own[k]
    copies_3 = []
    for k, (o, peer) in enumerate(zip((1, 2, 3), group_peers)):
        to = lax.rem(x + o, 4)
        copies_3.append(
            pltpu.make_async_remote_copy(
                src_ref=back.at[to],
                dst_ref=below.at[pl.ds(pl.multiple_of(x * QUARTER, 8), QUARTER), :],
                send_sem=send_3.at[k],
                recv_sem=recv_3.at[k],
                device_id=peer,
                device_id_type=MESH,
            )
        )
    for copy in copies_3:
        copy.start()
    below[pl.ds(pl.multiple_of(x * QUARTER, 8), QUARTER), :] = back[x]
    for copy in copies_3:
        copy.wait_recv()
    for d, copy in zip(DIRECTIONS, copies_w):
        pl.when(exists(*d))(copy.wait_send)
    for d, copy in zip(across, copies_x):
        pl.when(exists(*d))(copy.wait_send)
    for copy in copies_1 + copies_2 + copies_3:
        copy.wait_send()


def body(tracer, crowding):
    vmem = pl.BlockSpec(memory_space=pltpu.VMEM)
    hbm = pl.BlockSpec(memory_space=pl.ANY)
    f32 = jnp.float32
    dma = pltpu.SemaphoreType.DMA
    end, here, below = pl.pallas_call(
        kernel,
        out_shape=(
            jax.ShapeDtypeStruct((NY, NX, M), f32),
            jax.ShapeDtypeStruct((NY, NX, M), f32),
            jax.ShapeDtypeStruct((NY, M), f32),
        ),
        in_specs=[hbm, hbm],
        out_specs=(vmem, vmem, vmem),
        scratch_shapes=[
            pltpu.VMEM((ROWS, PITCH, M), f32),
            pltpu.VMEM((ROWS, PITCH, M), f32),
            pltpu.VMEM((ROWS, PITCH, M), f32),
            pltpu.VMEM((ROWS, PITCH, M), f32),
            pltpu.VMEM((NY, M), f32),
            pltpu.VMEM((4, QUARTER, M), f32),
            pltpu.VMEM((8, QUARTER, M), f32),
            pltpu.VMEM((QUARTER, M), f32),
            pltpu.VMEM((4, QUARTER, M), f32),
            dma((2,)),
            dma((8,)), dma((8,)), dma((8,)), dma((8,)),
            dma((2,)), dma((2,)),
            dma((3,)), dma((3,)), dma((7,)), dma((7,)), dma((3,)), dma((3,)),
        ],
        compiler_params=pltpu.CompilerParams(
            collective_id=0, has_side_effects=True, vmem_limit_bytes=40 * 1024 * 1024
        ),
    )(tracer, crowding)
    potential = (here + below[:, None, :]) * (1.0 / 1024)
    return (potential, end)


def solution(mesh):
    spec = P("rows", "cols", None)
    return jax.shard_map(body, mesh=mesh, in_specs=(spec, spec), out_specs=(spec, spec), check_vma=False)
```

```python
import jax
import jax.numpy as jnp
from jax import lax
from jax.experimental import pallas as pl
from jax.experimental.pallas import tpu as pltpu
from jax.sharding import PartitionSpec as P

NY, NX, M = 96, 32, 128
PITCH = 40
Y0 = 8
ROWS = NY + 2 * Y0
DY = 6
QUARTER = NY // 4
MESH = pl.DeviceIdType.MESH
DIRECTIONS = [(dr, dc) for dr in (-1, 0, 1) for dc in (-1, 0, 1) if (dr, dc) != (0, 0)]


CHUNKS = 4
A_ENDS = (31, 55, 79, NY + DY)
B_ENDS = (30, 54, 78, NY + DY)
MAIN = (0, 32, 56, 80, NY)
COUNT = 96


def kernel(
    tracer, crowding, end, here, below,
    u, v, w, w_deep, t2, tot, p1, p2, group,
    in_sem, send_sems, recv_sems, chain,
):
    r = lax.axis_index("rows")
    c = lax.axis_index("cols")
    n_r, n_c = 4, 32
    x = lax.rem(c, 4)
    g = lax.div(c, 4)
    z = lax.div(g, 2)
    interior = lambda ref: ref.at[Y0 : Y0 + NY, 0:NX, :]
    load_t = pltpu.make_async_copy(tracer, interior(u), in_sem.at[0])
    load_w = pltpu.make_async_copy(crowding, interior(w), in_sem.at[1])
    load_t.start()
    load_w.start()

    def exists(dr, dc):
        ok = None
        for there in ((r > 0) if dr < 0 else (r < n_r - 1) if dr > 0 else None,
                      (c > 0) if dc < 0 else (c < n_c - 1) if dc > 0 else None):
            if there is not None:
                ok = there if ok is None else ok & there
        return ok

    def neighbour(dr, dc):
        return {"rows": r + dr, "cols": c + dc}

    barrier = pltpu.get_barrier_semaphore()
    group_peers = [{"rows": r, "cols": g * 4 + lax.rem(x + o, 4)} for o in (1, 2, 3)]
    partner = {"rows": r, "cols": (z * 2 + 1 - lax.rem(g, 2)) * 4 + x}
    greeted = [(exists(*d), neighbour(*d)) for d in DIRECTIONS]
    greeted += [(z > 0, {"rows": r, "cols": c - 8}), (z < 3, {"rows": r, "cols": c + 8})]
    expected = jnp.int32(4)
    for peer in group_peers + [partner]:
        pl.semaphore_signal(barrier, inc=1, device_id=peer, device_id_type=MESH)
    for ok, peer in greeted:
        expected = expected + ok.astype(jnp.int32)

        @pl.when(ok)
        def _(peer=peer):
            pl.semaphore_signal(barrier, inc=1, device_id=peer, device_id_type=MESH)

    is_left, is_right, is_top, is_bottom = c == 0, c == n_c - 1, r == 0, r == n_r - 1
    flat = lambda ref: ref.reshape(ROWS * PITCH, M)
    fu, fv, fw, f2 = flat(u), flat(v), flat(w), flat(t2)

    def zero_sides(f, low, high):
        zero = jnp.zeros((high - low, M), jnp.float32)

        @pl.when(is_left)
        def _():
            f[pl.ds((Y0 + low) * PITCH - 1, high - low, stride=PITCH), :] = zero

        @pl.when(is_right)
        def _():
            f[pl.ds((Y0 + low) * PITCH + NX, high - low, stride=PITCH), :] = zero

    def zero_rows(f, low, high, halo=True):
        before, width = (4, PITCH) if halo else (0, NX)
        zero = jnp.zeros((width, M), jnp.float32)
        for edge, row in ((is_top, -1), (is_bottom, NY)):
            if low <= row < high:

                @pl.when(edge)
                def _(row=row):
                    f[pl.ds((Y0 + row) * PITCH - before, width), :] = zero

    zero_sides(fu, -DY, NY + DY)
    zero_sides(f2, -DY, NY + DY)
    zero_rows(fu, -DY, NY + DY)

    sent = []
    used = [0]

    def copy_to(source, target, peer):
        k = used[0]
        used[0] += 1
        return pltpu.make_async_remote_copy(
            src_ref=source, dst_ref=target, send_sem=send_sems.at[k], recv_sem=recv_sems.at[k],
            device_id=peer, device_id_type=MESH,
        )

    def halo(ref, rows, cols, dr, dc):
        (y1, y2), (x1, x2) = rows, cols
        down, aside = -dr * NY, 0
        if dc < 0:
            aside = NX
        if dc > 0:
            down, aside = down - 1, PITCH - NX
        source = ref.at[Y0 + y1 : Y0 + y2, x1:x2, :]
        target = ref.at[Y0 + y1 + down : Y0 + y2 + down, x1 + aside : x2 + aside, :]
        return exists(dr, dc), exists(-dr, -dc), copy_to(source, target, neighbour(dr, dc))

    def when(ok, do):
        if ok is None:
            do()
        else:
            pl.when(ok)(do)

    def start(items):
        for goes, _, copy in items:
            when(goes, copy.start)
            sent.append((goes, copy))

    def arrive(items):
        for _, comes, copy in items:
            when(comes, copy.wait_recv)

    def finish(count=None):
        for goes, copy in sent[:count]:
            when(goes, copy.wait_send)
        del sent[:count]

    load_t.wait()
    load_w.wait()
    pl.semaphore_wait(barrier, expected)

    def edge_cols(dc, low, high):
        return (low, high) if dc < 0 else (NX - high, NX - low)

    def from_row_neighbour(dr):
        t_rows = (0, DY) if dr < 0 else (NY - DY, NY)
        w_rows = (0, DY - 1) if dr < 0 else (NY - DY + 1, NY)
        out = [halo(u, t_rows, (0, NX), dr, 0), halo(w, w_rows, (0, NX), dr, 0)]
        for dc in (-1, 1):
            out.append(halo(u, t_rows, edge_cols(dc, 0, 2), dr, dc))
            out.append(halo(w, w_rows, edge_cols(dc, 0, 3), dr, dc))
        return out

    from_below = from_row_neighbour(-1)
    from_above = from_row_neighbour(1)
    first = []
    for j in range(CHUNKS):
        rows = (MAIN[j], MAIN[j + 1])
        first.append(
            [halo(u, rows, edge_cols(dc, 0, 2), 0, dc) for dc in (-1, 1)]
            + [halo(w, rows, edge_cols(dc, 0, 1), 0, dc) for dc in (-1, 1)]
        )
    deeper = [
        (exists(0, dc), exists(0, -dc), copy_to(
            w.at[Y0 : Y0 + NY, 1:3, :] if dc < 0 else w.at[Y0 : Y0 + NY, NX - 3 : NX - 1, :],
            w_deep.at[Y0 : Y0 + NY, 1:3, :] if dc < 0 else w_deep.at[Y0 - 1 : Y0 + NY - 1, 5:7, :],
            neighbour(0, dc),
        ))
        for dc in (-1, 1)
    ]
    start(from_above)
    start(first[0])
    start(from_below)
    for items in first[1:] + [deeper]:
        start(items)
    first_sends = len(sent)

    @pl.when(z < 3)
    def _():
        pl.semaphore_wait(chain, 1)

    @pl.when(z > 0)
    def _():
        pl.semaphore_signal(chain, inc=1, device_id={"rows": r, "cols": c - 8}, device_id_type=MESH)

    def step(src, low, high, tiles, store, first=False, last=False):
        def body(i, carry):
            north, centre = carry
            base = pl.multiple_of((Y0 + low + i) * PITCH, 8)
            south, new = [], []
            for k in range(tiles):
                at = base + 8 * k
                s = src[pl.ds(pl.multiple_of(at + PITCH, 8), 8), :]
                left = src[pl.ds(at - 1, 8), :]
                right = src[pl.ds(at + 1, 8), :]
                cr = fw[pl.ds(pl.multiple_of(at, 8), 8), :]
                spread = (left + right) + (north[k] + s)
                taken = centre[k] * cr
                if first:
                    taken = taken + taken
                grown = spread + centre[k] * (8.0 - taken)
                new.append(grown * (0.2 if first else 0.05 if last else 0.1))
                south.append(s)
            store(low + i, base, new)
            return tuple(centre), tuple(south)

        at = (Y0 + low - 1) * PITCH
        north = tuple(src[pl.ds(at + 8 * k, 8), :] for k in range(tiles))
        centre = tuple(src[pl.ds(at + PITCH + 8 * k, 8), :] for k in range(tiles))
        lax.fori_loop(0, high - low, body, (north, centre), unroll=2)

    def store_to(dst):
        def store(row, base, new):
            for k, value in enumerate(new):
                dst[pl.ds(pl.multiple_of(base + 8 * k, 8), 8), :] = value

        return store

    def rows_at(ends, j, s):
        return (ends[j - 1] - s if j else s - DY), ends[j] - s

    place = lax.broadcasted_iota(jnp.int32, (8, M), 0)

    second = []
    for j in range(CHUNKS):
        if j == 0:
            arrive(from_above)
        if j == CHUNKS - 1:
            arrive(from_below)
        arrive(first[j])
        low, high = rows_at(A_ENDS, j, 1)
        step(fu, low, high, 5, store_to(fv), first=True)
        zero_sides(fv, low, high)
        zero_rows(fv, low, high)
        low, high = rows_at(A_ENDS, j, 2)
        step(fv, low, high, 4, store_to(f2))
        zero_rows(f2, low, high, False)
        items = [halo(t2, (low, high), edge_cols(dc, 0, 4), 0, dc) for dc in (-1, 1)]
        start(items)
        second.append(items)
    arrive(deeper)
    finish(first_sends)

    def merge(row, low, high):
        mask = (place > low) & (place < high)
        w[row, NX:PITCH, :] = jnp.where(mask, w_deep[row], w[row, NX:PITCH, :])

    def merge_row(i, _):
        merge(i, 0, 7)
        return 0

    merge(Y0 - 1, 4, 7)
    lax.fori_loop(Y0, Y0 + NY - 1, merge_row, 0, unroll=5)
    merge(Y0 + NY - 1, 0, 4)

    def store_end(row, base, new):
        for k, value in enumerate(new):
            end[row, 8 * k : 8 * k + 8, :] = value
        total = (new[0] + new[1]) + (new[2] + new[3])
        tot[pl.ds(row, 1), :] = jnp.sum(total, axis=0, keepdims=True)

    def running(i, _):
        carry = jnp.zeros((1, M), jnp.float32)
        for k in range(4):
            value = end[i, 8 * k : 8 * k + 8, :]
            for shift in (1, 2, 4):
                value = value + jnp.where(place >= shift, pltpu.roll(value, shift, 0), 0.0)
            value = value + carry
            here[i, 8 * k : 8 * k + 8, :] = value
            carry = value[7:8, :]
        return 0

    def quarter(j):
        return pl.ds(j * QUARTER, QUARTER)

    def group_sum(j):
        arrive(totals[j])
        own = [p1[k, quarter(j), :] for k in range(4)]
        group[quarter(j), :] = (own[0] + own[1]) + (own[2] + own[3])
        items = [
            (g + k < 8, g >= k, copy_to(group.at[quarter(j), :], p2.at[g, quarter(j), :], {"rows": r, "cols": c + 4 * k}))
            for k in range(1, 8)
        ]
        start(items)
        return items

    totals, groups = [], []
    for j in range(CHUNKS):
        arrive(second[j])
        low, high = rows_at(B_ENDS, j, 3)
        step(f2, low, high, 5, store_to(fv))
        zero_sides(fv, low, high)
        zero_rows(fv, low, high)
        low, high = rows_at(B_ENDS, j, 4)
        step(fv, low, high, 5, store_to(fu))
        zero_sides(fu, low, high)
        zero_rows(fu, low, high)
        low, high = rows_at(B_ENDS, j, 5)
        step(fu, low, high, 5, store_to(fv))
        zero_sides(fv, low, high)
        zero_rows(fv, low, high)
        low, high = rows_at(B_ENDS, j, 6)
        step(fv, low, high, 4, store_end, last=True)
        items = [(None, None, copy_to(tot.at[quarter(j), :], p1.at[x, quarter(j), :], peer)) for peer in group_peers]
        start(items)
        totals.append(items)
        p1[x, quarter(j), :] = tot[quarter(j), :]
        if j:
            groups.append(group_sum(j - 1))
        lax.fori_loop(low, high, running, 0, unroll=2)
    groups.append(group_sum(CHUNKS - 1))
    for j in range(CHUNKS):
        arrive(groups[j])
        before = jnp.zeros((QUARTER, M), jnp.float32)
        for k in range(7):
            before = before + jnp.where(k < g, p2[k, quarter(j), :], 0.0)
        for k in range(3):
            before = before + jnp.where(k < x, p1[k, quarter(j), :], 0.0)
        below[quarter(j), :] = before
    finish()

def body(tracer, crowding):
    vmem = pl.BlockSpec(memory_space=pltpu.VMEM)
    hbm = pl.BlockSpec(memory_space=pltpu.HBM)
    f32 = jnp.float32
    dma = pltpu.SemaphoreType.DMA
    end, here, below = pl.pallas_call(
        kernel,
        out_shape=(
            jax.ShapeDtypeStruct((NY, NX, M), f32),
            jax.ShapeDtypeStruct((NY, NX, M), f32),
            jax.ShapeDtypeStruct((NY, M), f32),
        ),
        in_specs=[hbm, hbm],
        out_specs=(vmem, vmem, vmem),
        scratch_shapes=[
            pltpu.VMEM((ROWS, PITCH, M), f32),
            pltpu.VMEM((ROWS, PITCH, M), f32),
            pltpu.VMEM((ROWS, PITCH, M), f32),
            pltpu.VMEM((ROWS, 8, M), f32),
            pltpu.VMEM((ROWS, PITCH, M), f32),
            pltpu.VMEM((NY, M), f32),
            pltpu.VMEM((4, NY, M), f32),
            pltpu.VMEM((8, NY, M), f32),
            pltpu.VMEM((NY, M), f32),
            dma((2,)), dma((COUNT,)), dma((COUNT,)),
            pltpu.SemaphoreType.REGULAR,
        ],
        compiler_params=pltpu.CompilerParams(
            collective_id=0, has_side_effects=True, vmem_limit_bytes=50 * 1024 * 1024
        ),
    )(tracer, crowding)
    potential = (here + below[:, None, :]) * (1.0 / 1024)
    return (potential, end)


def solution(mesh):
    spec = P("rows", "cols", None)
    return jax.shard_map(body, mesh=mesh, in_specs=(spec, spec), out_specs=(spec, spec), check_vma=False)
```

```python
import functools

import jax
import jax.numpy as jnp
from jax import lax
from jax.experimental import pallas as pl
from jax.experimental.pallas import tpu as pltpu
from jax.sharding import PartitionSpec as P

NY, NX, M = 96, 32, 128
PITCH = 40
Y0 = 8
ROWS = NY + 2 * Y0
DY = 6
QUARTER = NY // 4
MESH = pl.DeviceIdType.MESH
DIRECTIONS = [(dr, dc) for dr in (-1, 0, 1) for dc in (-1, 0, 1) if (dr, dc) != (0, 0)]


CHUNKS = 4
CAP = CHUNKS
A_ENDS = (37, 61, 85, NY + DY)
B_ENDS = (36, 60, 84, NY + DY)
MAIN = (0, 38, 62, 86, NY)
COUNT = 96


def kernel(
    tracer, crowding, end, here, below,
    u, v, w, w_deep, t2, tot, p1, p2, group,
    in_sem, send_sems, recv_sems, chain,
):
    r = lax.axis_index("rows")
    c = lax.axis_index("cols")
    n_r, n_c = 4, 32
    x = lax.rem(c, 4)
    g = lax.div(c, 4)
    z = lax.div(g, 2)
    interior = lambda ref: ref.at[Y0 : Y0 + NY, 0:NX, :]
    load_t = pltpu.make_async_copy(tracer, interior(u), in_sem.at[0])
    load_w = pltpu.make_async_copy(crowding, interior(w), in_sem.at[1])
    load_t.start()
    load_w.start()

    def exists(dr, dc):
        ok = None
        for there in ((r > 0) if dr < 0 else (r < n_r - 1) if dr > 0 else None,
                      (c > 0) if dc < 0 else (c < n_c - 1) if dc > 0 else None):
            if there is not None:
                ok = there if ok is None else ok & there
        return ok

    def neighbour(dr, dc):
        return {"rows": r + dr, "cols": c + dc}

    barrier = pltpu.get_barrier_semaphore()
    group_peers = [{"rows": r, "cols": g * 4 + lax.rem(x + o, 4)} for o in (1, 2, 3)]
    partner = {"rows": r, "cols": (z * 2 + 1 - lax.rem(g, 2)) * 4 + x}
    greeted = [(exists(*d), neighbour(*d)) for d in DIRECTIONS]
    greeted += [(z > 0, {"rows": r, "cols": c - 8}), (z < 3, {"rows": r, "cols": c + 8})]
    expected = jnp.int32(4)
    for peer in group_peers + [partner]:
        pl.semaphore_signal(barrier, inc=1, device_id=peer, device_id_type=MESH)
    for ok, peer in greeted:
        expected = expected + ok.astype(jnp.int32)

        @pl.when(ok)
        def _(peer=peer):
            pl.semaphore_signal(barrier, inc=1, device_id=peer, device_id_type=MESH)

    is_left, is_right, is_top, is_bottom = c == 0, c == n_c - 1, r == 0, r == n_r - 1
    flat = lambda ref: ref.reshape(ROWS * PITCH, M)
    fu, fv, fw, f2 = flat(u), flat(v), flat(w), flat(t2)

    def zero_sides(f, low, high):
        zero = jnp.zeros((high + 1 - low, M), jnp.float32)

        @pl.when(is_left)
        def _():
            f[pl.ds((Y0 + low) * PITCH - 1, high + 1 - low, stride=PITCH), :] = zero

        @pl.when(is_right)
        def _():
            f[pl.ds((Y0 + low) * PITCH + NX, high + 1 - low, stride=PITCH), :] = zero

    def zero_rows(f, low, high, halo=True):
        before, width = (4, PITCH) if halo else (0, NX)
        zero = jnp.zeros((width, M), jnp.float32)
        for edge, row in ((is_top, -1), (is_bottom, NY)):
            if low <= row < high:

                @pl.when(edge)
                def _(row=row):
                    f[pl.ds((Y0 + row) * PITCH - before, width), :] = zero

    zero_sides(fu, -DY, NY + DY)
    zero_sides(f2, -DY, NY + DY)
    zero_rows(fu, -DY, NY + DY)

    sent = []
    used = [0]

    def copy_to(source, target, peer):
        k = used[0]
        used[0] += 1
        return pltpu.make_async_remote_copy(
            src_ref=source, dst_ref=target, send_sem=send_sems.at[k], recv_sem=recv_sems.at[k],
            device_id=peer, device_id_type=MESH,
        )

    def halo(ref, rows, cols, dr, dc):
        (y1, y2), (x1, x2) = rows, cols
        down, aside = -dr * NY, 0
        if dc < 0:
            aside = NX
        if dc > 0:
            down, aside = down - 1, PITCH - NX
        source = ref.at[Y0 + y1 : Y0 + y2, x1:x2, :]
        target = ref.at[Y0 + y1 + down : Y0 + y2 + down, x1 + aside : x2 + aside, :]
        return exists(dr, dc), exists(-dr, -dc), copy_to(source, target, neighbour(dr, dc))

    def when(ok, do):
        if ok is None:
            do()
        else:
            pl.when(ok)(do)

    def start(items):
        for goes, _, copy in items:
            when(goes, copy.start)
            sent.append((goes, copy))

    def arrive(items):
        for _, comes, copy in items:
            when(comes, copy.wait_recv)

    def finish(count=None):
        for goes, copy in sent[:count]:
            when(goes, copy.wait_send)
        del sent[:count]

    load_t.wait()
    load_w.wait()
    pl.semaphore_wait(barrier, expected)

    def edge_cols(dc, low, high):
        return (low, high) if dc < 0 else (NX - high, NX - low)

    def from_row_neighbour(dr):
        t_rows = (0, DY) if dr < 0 else (NY - DY, NY)
        w_rows = (0, DY - 1) if dr < 0 else (NY - DY + 1, NY)
        out = [halo(u, t_rows, (0, NX), dr, 0), halo(w, w_rows, (0, NX), dr, 0)]
        for dc in (-1, 1):
            out.append(halo(u, t_rows, edge_cols(dc, 0, 2), dr, dc))
            out.append(halo(w, w_rows, edge_cols(dc, 0, 3), dr, dc))
        return out

    from_below = from_row_neighbour(-1)
    from_above = from_row_neighbour(1)
    first = []
    for j in range(CHUNKS):
        rows = (MAIN[j], MAIN[j + 1])
        first.append(
            [halo(u, rows, edge_cols(dc, 0, 2), 0, dc) for dc in (-1, 1)]
            + [halo(w, rows, edge_cols(dc, 0, 1), 0, dc) for dc in (-1, 1)]
        )
    deeper = [
        (exists(0, dc), exists(0, -dc), copy_to(
            w.at[Y0 : Y0 + NY, 1:3, :] if dc < 0 else w.at[Y0 : Y0 + NY, NX - 3 : NX - 1, :],
            w_deep.at[Y0 : Y0 + NY, 1:3, :] if dc < 0 else w_deep.at[Y0 - 1 : Y0 + NY - 1, 5:7, :],
            neighbour(0, dc),
        ))
        for dc in (-1, 1)
    ]
    start(from_above)
    start(first[0])
    start(from_below)
    for items in first[1:] + [deeper]:
        start(items)
    first_sends = len(sent)


    def chain_stage(k):
        if k > 0:

            @pl.when(z < 3)
            def _():
                pl.semaphore_wait(chain.at[k - 1], 1)

        if k < 3:

            @pl.when(z > 0)
            def _():
                pl.semaphore_signal(chain.at[k], inc=1, device_id={"rows": r, "cols": c - 8}, device_id_type=MESH)

    chain_stage(0)

    def step(src, low, high, tiles, store, first=False, last=False):
        def body(i, carry):
            north, centre = carry
            base = pl.multiple_of((Y0 + low + i) * PITCH, 8)
            south, new = [], []
            for k in range(tiles):
                at = base + 8 * k
                s = src[pl.ds(pl.multiple_of(at + PITCH, 8), 8), :]
                left = src[pl.ds(at - 1, 8), :]
                right = src[pl.ds(at + 1, 8), :]
                cr = fw[pl.ds(pl.multiple_of(at, 8), 8), :]
                spread = (left + right) + (north[k] + s)
                taken = centre[k] * cr
                if first:
                    taken = taken + taken
                grown = spread + centre[k] * (8.0 - taken)
                new.append(grown * (0.2 if first else 0.05 if last else 0.1))
                south.append(s)
            store(low + i, base, new)
            return tuple(centre), tuple(south)

        at = (Y0 + low - 1) * PITCH
        north = tuple(src[pl.ds(at + 8 * k, 8), :] for k in range(tiles))
        centre = tuple(src[pl.ds(at + PITCH + 8 * k, 8), :] for k in range(tiles))
        lax.fori_loop(0, high - low, body, (north, centre), unroll=2)

    def store_to(dst):
        def store(row, base, new):
            for k, value in enumerate(new):
                dst[pl.ds(pl.multiple_of(base + 8 * k, 8), 8), :] = value

        return store

    def rows_at(ends, j, s):
        if j == CAP:
            return s - DY, s
        return (ends[j - 1] - s if j else s), ends[j] - s

    place = lax.broadcasted_iota(jnp.int32, (8, M), 0)

    second = []
    for j in range(CHUNKS + 1):
        if j == CAP:
            arrive(from_above)
        else:
            arrive(first[j])
        if j == CHUNKS - 1:
            arrive(from_below)
        low, high = rows_at(A_ENDS, j, 1)
        step(fu, low, high, 5, store_to(fv), first=True)
        zero_sides(fv, low, high)
        zero_rows(fv, low, high)
        low, high = rows_at(A_ENDS, j, 2)
        step(fv, low, high, 4, store_to(f2))
        zero_rows(f2, low, high, False)
        items = [halo(t2, (low, high), edge_cols(dc, 0, 4), 0, dc) for dc in (-1, 1)]
        start(items)
        second.append(items)
        if j in (0, 2):
            chain_stage(1 + j // 2)
    arrive(deeper)
    finish(first_sends)

    def merge(row, low, high):
        mask = (place > low) & (place < high)
        w[row, NX:PITCH, :] = jnp.where(mask, w_deep[row], w[row, NX:PITCH, :])

    def merge_row(i, _):
        merge(i, 0, 7)
        return 0

    merge(Y0 - 1, 4, 7)
    lax.fori_loop(Y0, Y0 + NY - 1, merge_row, 0, unroll=5)
    merge(Y0 + NY - 1, 0, 4)

    def store_end(row, base, new, first_row):
        for k, value in enumerate(new):
            end[row, 8 * k : 8 * k + 8, :] = value
        total = (new[0] + new[1]) + (new[2] + new[3])
        tot[pl.ds(row - DY if first_row >= DY else row + NY - DY, 1), :] = jnp.sum(total, axis=0, keepdims=True)

    def running(i, _):
        carry = jnp.zeros((1, M), jnp.float32)
        for k in range(4):
            value = end[i, 8 * k : 8 * k + 8, :]
            for shift in (1, 2, 4):
                value = value + jnp.where(place >= shift, pltpu.roll(value, shift, 0), 0.0)
            value = value + carry
            here[i, 8 * k : 8 * k + 8, :] = value
            carry = value[7:8, :]
        return 0

    def quarter(j):
        return pl.ds(j * QUARTER, QUARTER)

    def group_sum(j):
        arrive(totals[j])
        own = [p1[k, quarter(j), :] for k in range(4)]
        group[quarter(j), :] = (own[0] + own[1]) + (own[2] + own[3])
        items = [
            (g + k < 8, g >= k, copy_to(group.at[quarter(j), :], p2.at[g, quarter(j), :], {"rows": r, "cols": c + 4 * k}))
            for k in range(1, 8)
        ]
        start(items)
        return items

    totals, groups = [], []
    for j in range(CHUNKS + 1):
        arrive(second[j])
        low, high = rows_at(B_ENDS, j, 3)
        step(f2, low, high, 5, store_to(fv))
        zero_sides(fv, low, high)
        zero_rows(fv, low, high)
        low, high = rows_at(B_ENDS, j, 4)
        step(fv, low, high, 5, store_to(fu))
        zero_sides(fu, low, high)
        zero_rows(fu, low, high)
        low, high = rows_at(B_ENDS, j, 5)
        step(fu, low, high, 5, store_to(fv))
        zero_sides(fv, low, high)
        zero_rows(fv, low, high)
        low, high = rows_at(B_ENDS, j, 6)
        step(fv, low, high, 4, functools.partial(store_end, first_row=low), last=True)
        if j == CHUNKS - 1:
            continue
        k = min(j, CHUNKS - 1)
        items = [(None, None, copy_to(tot.at[quarter(k), :], p1.at[x, quarter(k), :], peer)) for peer in group_peers]
        start(items)
        totals.append(items)
        p1[x, quarter(k), :] = tot[quarter(k), :]
    chain_stage(3)
    for j in range(CHUNKS):
        groups.append(group_sum(j))
    lax.fori_loop(0, NY, running, 0, unroll=2)
    for j in range(CHUNKS):
        arrive(groups[j])
        before = jnp.zeros((QUARTER, M), jnp.float32)
        for k in range(7):
            before = before + jnp.where(k < g, p2[k, quarter(j), :], 0.0)
        for k in range(3):
            before = before + jnp.where(k < x, p1[k, quarter(j), :], 0.0)
        at = DY + j * QUARTER
        if j < CHUNKS - 1:
            below[at : at + QUARTER, :] = before
        else:
            below[at:NY, :] = before[: NY - at]
            below[0:DY, :] = before[NY - at :]
    finish()

def body(tracer, crowding):
    vmem = pl.BlockSpec(memory_space=pltpu.VMEM)
    hbm = pl.BlockSpec(memory_space=pltpu.HBM)
    f32 = jnp.float32
    dma = pltpu.SemaphoreType.DMA
    end, here, below = pl.pallas_call(
        kernel,
        out_shape=(
            jax.ShapeDtypeStruct((NY, NX, M), f32),
            jax.ShapeDtypeStruct((NY, NX, M), f32),
            jax.ShapeDtypeStruct((NY, M), f32),
        ),
        in_specs=[hbm, hbm],
        out_specs=(vmem, vmem, vmem),
        scratch_shapes=[
            pltpu.VMEM((ROWS, PITCH, M), f32),
            pltpu.VMEM((ROWS, PITCH, M), f32),
            pltpu.VMEM((ROWS, PITCH, M), f32),
            pltpu.VMEM((ROWS, 8, M), f32),
            pltpu.VMEM((ROWS, PITCH, M), f32),
            pltpu.VMEM((NY, M), f32),
            pltpu.VMEM((4, NY, M), f32),
            pltpu.VMEM((8, NY, M), f32),
            pltpu.VMEM((NY, M), f32),
            dma((2,)), dma((COUNT,)), dma((COUNT,)),
            pltpu.SemaphoreType.REGULAR((3,)),
        ],
        compiler_params=pltpu.CompilerParams(
            collective_id=0, has_side_effects=True, vmem_limit_bytes=50 * 1024 * 1024
        ),
    )(tracer, crowding)
    potential = (here + below[:, None, :]) * (1.0 / 1024)
    return (potential, end)


def solution(mesh):
    spec = P("rows", "cols", None)
    return jax.shard_map(body, mesh=mesh, in_specs=(spec, spec), out_specs=(spec, spec), check_vma=False)
```

```python
import functools

import jax
import jax.numpy as jnp
from jax import lax
from jax.experimental import pallas as pl
from jax.experimental.pallas import tpu as pltpu
from jax.sharding import PartitionSpec as P

NY, NX, M = 96, 32, 128
PITCH = 40
Y0 = 8
ROWS = NY + 2 * Y0
DY = 6
QUARTER = NY // 4
MESH = pl.DeviceIdType.MESH
DIRECTIONS = [(dr, dc) for dr in (-1, 0, 1) for dc in (-1, 0, 1) if (dr, dc) != (0, 0)]


CHUNKS = 4
CAP = CHUNKS
A_ENDS = (37, 61, 85, NY + 2)
B_ENDS = (36, 60, 84, NY + DY)
MAIN = (0, 38, 62, 86, NY)
COUNT = 96


def kernel(
    tracer, crowding, end, here, below,
    u, v, w, w_deep, t2, tot, p1, p2, group,
    in_sem, send_sems, recv_sems, chain,
):
    r = lax.axis_index("rows")
    c = lax.axis_index("cols")
    n_r, n_c = 4, 32
    x = lax.rem(c, 4)
    g = lax.div(c, 4)
    z = lax.div(g, 2)
    interior = lambda ref: ref.at[Y0 : Y0 + NY, 0:NX, :]
    load_t = pltpu.make_async_copy(tracer, interior(u), in_sem.at[0])
    load_w = pltpu.make_async_copy(crowding, interior(w), in_sem.at[1])
    load_t.start()
    load_w.start()

    def exists(dr, dc):
        ok = None
        for there in ((r > 0) if dr < 0 else (r < n_r - 1) if dr > 0 else None,
                      (c > 0) if dc < 0 else (c < n_c - 1) if dc > 0 else None):
            if there is not None:
                ok = there if ok is None else ok & there
        return ok

    def neighbour(dr, dc):
        return {"rows": r + dr, "cols": c + dc}

    barrier = pltpu.get_barrier_semaphore()
    group_peers = [{"rows": r, "cols": g * 4 + lax.rem(x + o, 4)} for o in (1, 2, 3)]
    partner = {"rows": r, "cols": (z * 2 + 1 - lax.rem(g, 2)) * 4 + x}
    greeted = [(exists(*d), neighbour(*d)) for d in DIRECTIONS]
    greeted += [(z > 0, {"rows": r, "cols": c - 8}), (z < 3, {"rows": r, "cols": c + 8})]
    expected = jnp.int32(4)
    for peer in group_peers + [partner]:
        pl.semaphore_signal(barrier, inc=1, device_id=peer, device_id_type=MESH)
    for ok, peer in greeted:
        expected = expected + ok.astype(jnp.int32)

        @pl.when(ok)
        def _(peer=peer):
            pl.semaphore_signal(barrier, inc=1, device_id=peer, device_id_type=MESH)

    is_left, is_right, is_top, is_bottom = c == 0, c == n_c - 1, r == 0, r == n_r - 1
    flat = lambda ref: ref.reshape(ROWS * PITCH, M)
    fu, fv, fw, f2 = flat(u), flat(v), flat(w), flat(t2)

    def zero_sides(f, low, high):
        zero = jnp.zeros((high + 1 - low, M), jnp.float32)

        @pl.when(is_left)
        def _():
            f[pl.ds((Y0 + low) * PITCH - 1, high + 1 - low, stride=PITCH), :] = zero

        @pl.when(is_right)
        def _():
            f[pl.ds((Y0 + low) * PITCH + NX, high + 1 - low, stride=PITCH), :] = zero

    def zero_rows(f, low, high):
        zero = jnp.zeros((PITCH, M), jnp.float32)
        for edge, row in ((is_top, -1), (is_bottom, NY)):
            if low <= row < high:

                @pl.when(edge)
                def _(row=row):
                    f[pl.ds((Y0 + row) * PITCH - 4, PITCH), :] = zero

    zero_sides(fu, -DY, NY + DY)
    zero_sides(f2, -DY, NY + DY)
    zero_rows(fu, -DY, NY + DY)
    zero_rows(f2, -DY, NY + DY)

    sent = []
    used = [0]

    def copy_to(source, target, peer):
        k = used[0]
        used[0] += 1
        return pltpu.make_async_remote_copy(
            src_ref=source, dst_ref=target, send_sem=send_sems.at[k], recv_sem=recv_sems.at[k],
            device_id=peer, device_id_type=MESH,
        )

    def halo(ref, rows, cols, dr, dc):
        (y1, y2), (x1, x2) = rows, cols
        down, aside = -dr * NY, 0
        if dc < 0:
            aside = NX
        if dc > 0:
            down, aside = down - 1, PITCH - NX
        source = ref.at[Y0 + y1 : Y0 + y2, x1:x2, :]
        target = ref.at[Y0 + y1 + down : Y0 + y2 + down, x1 + aside : x2 + aside, :]
        return exists(dr, dc), exists(-dr, -dc), copy_to(source, target, neighbour(dr, dc))

    def when(ok, do):
        if ok is None:
            do()
        else:
            pl.when(ok)(do)

    def start(items):
        for goes, _, copy in items:
            when(goes, copy.start)
            sent.append((goes, copy))

    def arrive(items):
        for _, comes, copy in items:
            when(comes, copy.wait_recv)

    def finish(count=None):
        for goes, copy in sent[:count]:
            when(goes, copy.wait_send)
        del sent[:count]

    load_t.wait()
    load_w.wait()
    pl.semaphore_wait(barrier, expected)

    def edge_cols(dc, low, high):
        return (low, high) if dc < 0 else (NX - high, NX - low)

    def row_halo(ref, low, high, dr, dc, depth=None):
        rows = (low, high) if dr < 0 else (NY - high, NY - low)
        return halo(ref, rows, edge_cols(dc, 0, depth) if dc else (0, NX), dr, dc)

    def from_row_neighbour(dr):
        out = [row_halo(u, 0, 2, dr, 0), row_halo(w, 0, 1, dr, 0)]
        for dc in (-1, 1):
            out.append(row_halo(u, 0, 2, dr, dc, 2))
            out.append(row_halo(w, 0, 3, dr, dc, 3))
        return out

    def again_from_row_neighbour(dr):
        return [row_halo(t2, 0, 4, dr, dc, 4) for dc in (0, -1, 1)]

    from_below = from_row_neighbour(-1)
    from_above = from_row_neighbour(1)
    first = []
    for j in range(CHUNKS):
        rows = (MAIN[j], MAIN[j + 1])
        first.append(
            [halo(u, rows, edge_cols(dc, 0, 2), 0, dc) for dc in (-1, 1)]
            + [halo(w, rows, edge_cols(dc, 0, 1), 0, dc) for dc in (-1, 1)]
        )
    deeper = [
        (exists(0, dc), exists(0, -dc), copy_to(
            w.at[Y0 : Y0 + NY, 1:3, :] if dc < 0 else w.at[Y0 : Y0 + NY, NX - 3 : NX - 1, :],
            w_deep.at[Y0 : Y0 + NY, 1:3, :] if dc < 0 else w_deep.at[Y0 - 1 : Y0 + NY - 1, 5:7, :],
            neighbour(0, dc),
        ))
        for dc in (-1, 1)
    ] + [row_halo(w, 1, 3, dr, 0) for dr in (-1, 1)]
    start(from_above)
    start(from_below)
    start(first[0])
    for items in first[1:] + [deeper]:
        start(items)
    first_sends = len(sent)


    def chain_stage(k):
        if k > 0:

            @pl.when(z < 3)
            def _():
                pl.semaphore_wait(chain.at[k - 1], 1)

        if k < 3:

            @pl.when(z > 0)
            def _():
                pl.semaphore_signal(chain.at[k], inc=1, device_id={"rows": r, "cols": c - 8}, device_id_type=MESH)

    chain_stage(0)

    def step(src, low, high, tiles, store, first=False, last=False):
        def body(i, carry):
            north, centre = carry
            base = pl.multiple_of((Y0 + low + i) * PITCH, 8)
            south, new = [], []
            for k in range(tiles):
                at = base + 8 * k
                s = src[pl.ds(pl.multiple_of(at + PITCH, 8), 8), :]
                left = src[pl.ds(at - 1, 8), :]
                right = src[pl.ds(at + 1, 8), :]
                cr = fw[pl.ds(pl.multiple_of(at, 8), 8), :]
                spread = (left + right) + (north[k] + s)
                taken = centre[k] * cr
                if first:
                    taken = taken + taken
                grown = spread + centre[k] * (8.0 - taken)
                new.append(grown * (0.2 if first else 0.05 if last else 0.1))
                south.append(s)
            store(low + i, base, new)
            return tuple(centre), tuple(south)

        at = (Y0 + low - 1) * PITCH
        north = tuple(src[pl.ds(at + 8 * k, 8), :] for k in range(tiles))
        centre = tuple(src[pl.ds(at + PITCH + 8 * k, 8), :] for k in range(tiles))
        lax.fori_loop(0, high - low, body, (north, centre), unroll=2)

    def store_to(dst):
        def store(row, base, new):
            for k, value in enumerate(new):
                dst[pl.ds(pl.multiple_of(base + 8 * k, 8), 8), :] = value

        return store

    def rows_at(ends, j, s):
        if j == CAP:
            return s - ends[CHUNKS - 1] + NY, s
        return (ends[j - 1] - s if j else s), ends[j] - s

    place = lax.broadcasted_iota(jnp.int32, (8, M), 0)

    second = []
    for j in range(CHUNKS + 1):
        if j == CAP:
            arrive(from_above)
        else:
            arrive(first[j])
        if j == CHUNKS - 1:
            arrive(from_below)
        low, high = rows_at(A_ENDS, j, 1)
        step(fu, low, high, 5, store_to(fv), first=True)
        zero_sides(fv, low, high)
        zero_rows(fv, low, high)
        low, high = rows_at(A_ENDS, j, 2)
        step(fv, low, high, 4, store_to(f2))
        items = [halo(t2, (low, high), edge_cols(dc, 0, 4), 0, dc) for dc in (-1, 1)]
        start(items)
        second.append(items)
        if j == CHUNKS - 1:
            again_from_above = again_from_row_neighbour(1)
            start(again_from_above)
        if j == CAP:
            again_from_below = again_from_row_neighbour(-1)
            start(again_from_below)
        if j in (0, 2):
            chain_stage(1 + j // 2)
    arrive(deeper)
    finish(first_sends)

    def merge(row, low, high):
        mask = (place > low) & (place < high)
        w[row, NX:PITCH, :] = jnp.where(mask, w_deep[row], w[row, NX:PITCH, :])

    def merge_row(i, _):
        merge(i, 0, 7)
        return 0

    merge(Y0 - 1, 4, 7)
    lax.fori_loop(Y0, Y0 + NY - 1, merge_row, 0, unroll=5)
    merge(Y0 + NY - 1, 0, 4)

    def store_end(row, base, new, first_row):
        for k, value in enumerate(new):
            end[row, 8 * k : 8 * k + 8, :] = value
        total = (new[0] + new[1]) + (new[2] + new[3])
        tot[pl.ds(row - DY if first_row >= DY else row + NY - DY, 1), :] = jnp.sum(total, axis=0, keepdims=True)

    def running(i, _):
        carry = jnp.zeros((1, M), jnp.float32)
        for k in range(4):
            value = end[i, 8 * k : 8 * k + 8, :]
            for shift in (1, 2, 4):
                value = value + jnp.where(place >= shift, pltpu.roll(value, shift, 0), 0.0)
            value = value + carry
            here[i, 8 * k : 8 * k + 8, :] = value
            carry = value[7:8, :]
        return 0

    def quarter(j):
        return pl.ds(j * QUARTER, QUARTER)

    def group_sum(j):
        arrive(totals[j])
        own = [p1[k, quarter(j), :] for k in range(4)]
        group[quarter(j), :] = (own[0] + own[1]) + (own[2] + own[3])
        items = [
            (g + k < 8, g >= k, copy_to(group.at[quarter(j), :], p2.at[g, quarter(j), :], {"rows": r, "cols": c + 4 * k}))
            for k in range(1, 8)
        ]
        start(items)
        return items

    totals, groups = [], []
    for j in range(CHUNKS + 1):
        arrive(second[j])
        if j == CHUNKS - 1:
            arrive(again_from_below)
        if j == CAP:
            arrive(again_from_above)
        low, high = rows_at(B_ENDS, j, 3)
        step(f2, low, high, 5, store_to(fv))
        zero_sides(fv, low, high)
        zero_rows(fv, low, high)
        low, high = rows_at(B_ENDS, j, 4)
        step(fv, low, high, 5, store_to(fu))
        zero_sides(fu, low, high)
        zero_rows(fu, low, high)
        low, high = rows_at(B_ENDS, j, 5)
        step(fu, low, high, 5, store_to(fv))
        zero_sides(fv, low, high)
        zero_rows(fv, low, high)
        low, high = rows_at(B_ENDS, j, 6)
        step(fv, low, high, 4, functools.partial(store_end, first_row=low), last=True)
        if j == CHUNKS - 1:
            continue
        k = min(j, CHUNKS - 1)
        items = [(None, None, copy_to(tot.at[quarter(k), :], p1.at[x, quarter(k), :], peer)) for peer in group_peers]
        start(items)
        totals.append(items)
        p1[x, quarter(k), :] = tot[quarter(k), :]
    chain_stage(3)
    for j in range(CHUNKS):
        groups.append(group_sum(j))
    lax.fori_loop(0, NY, running, 0, unroll=2)
    for j in range(CHUNKS):
        arrive(groups[j])
        before = jnp.zeros((QUARTER, M), jnp.float32)
        for k in range(7):
            before = before + jnp.where(k < g, p2[k, quarter(j), :], 0.0)
        for k in range(3):
            before = before + jnp.where(k < x, p1[k, quarter(j), :], 0.0)
        at = DY + j * QUARTER
        if j < CHUNKS - 1:
            below[at : at + QUARTER, :] = before
        else:
            below[at:NY, :] = before[: NY - at]
            below[0:DY, :] = before[NY - at :]
    finish()

def body(tracer, crowding):
    vmem = pl.BlockSpec(memory_space=pltpu.VMEM)
    hbm = pl.BlockSpec(memory_space=pltpu.HBM)
    f32 = jnp.float32
    dma = pltpu.SemaphoreType.DMA
    end, here, below = pl.pallas_call(
        kernel,
        out_shape=(
            jax.ShapeDtypeStruct((NY, NX, M), f32),
            jax.ShapeDtypeStruct((NY, NX, M), f32),
            jax.ShapeDtypeStruct((NY, M), f32),
        ),
        in_specs=[hbm, hbm],
        out_specs=(vmem, vmem, vmem),
        scratch_shapes=[
            pltpu.VMEM((ROWS, PITCH, M), f32),
            pltpu.VMEM((ROWS, PITCH, M), f32),
            pltpu.VMEM((ROWS, PITCH, M), f32),
            pltpu.VMEM((ROWS, 8, M), f32),
            pltpu.VMEM((ROWS, PITCH, M), f32),
            pltpu.VMEM((NY, M), f32),
            pltpu.VMEM((4, NY, M), f32),
            pltpu.VMEM((8, NY, M), f32),
            pltpu.VMEM((NY, M), f32),
            dma((2,)), dma((COUNT,)), dma((COUNT,)),
            pltpu.SemaphoreType.REGULAR((3,)),
        ],
        compiler_params=pltpu.CompilerParams(
            collective_id=0, has_side_effects=True, vmem_limit_bytes=50 * 1024 * 1024
        ),
    )(tracer, crowding)
    potential = (here + below[:, None, :]) * (1.0 / 1024)
    return (potential, end)


def solution(mesh):
    spec = P("rows", "cols", None)
    return jax.shard_map(body, mesh=mesh, in_specs=(spec, spec), out_specs=(spec, spec), check_vma=False)
```

```python
import functools

import jax
import jax.numpy as jnp
from jax import lax
from jax.experimental import pallas as pl
from jax.experimental.pallas import tpu as pltpu
from jax.sharding import PartitionSpec as P

NY, NX, M = 96, 32, 128
PITCH = 40
Y0 = 8
ROWS = NY + 2 * Y0
DY = 6
QUARTER = NY // 4
MESH = pl.DeviceIdType.MESH
DIRECTIONS = [(dr, dc) for dr in (-1, 0, 1) for dc in (-1, 0, 1) if (dr, dc) != (0, 0)]


CHUNKS = 4
CAP = CHUNKS
A_ENDS = (37, 61, 85, NY + 3)
B_ENDS = (36, 60, 84, NY + DY)
MAIN = (0, 38, 62, 86, NY)
COUNT = 96


def kernel(
    tracer, crowding, end, here, below,
    u, v, w, u2, t3, tot, p1, p2, group,
    in_sem, send_sems, recv_sems, chain,
):
    r = lax.axis_index("rows")
    c = lax.axis_index("cols")
    n_r, n_c = 4, 32
    x = lax.rem(c, 4)
    g = lax.div(c, 4)
    z = lax.div(g, 2)
    interior = lambda ref: ref.at[Y0 : Y0 + NY, 0:NX, :]
    load_t = pltpu.make_async_copy(tracer, interior(u), in_sem.at[0])
    load_w = pltpu.make_async_copy(crowding, interior(w), in_sem.at[1])
    load_t.start()
    load_w.start()

    def exists(dr, dc):
        ok = None
        for there in ((r > 0) if dr < 0 else (r < n_r - 1) if dr > 0 else None,
                      (c > 0) if dc < 0 else (c < n_c - 1) if dc > 0 else None):
            if there is not None:
                ok = there if ok is None else ok & there
        return ok

    def neighbour(dr, dc):
        return {"rows": r + dr, "cols": c + dc}

    barrier = pltpu.get_barrier_semaphore()
    group_peers = [{"rows": r, "cols": g * 4 + lax.rem(x + o, 4)} for o in (1, 2, 3)]
    partner = {"rows": r, "cols": (z * 2 + 1 - lax.rem(g, 2)) * 4 + x}
    greeted = [(exists(*d), neighbour(*d)) for d in DIRECTIONS]
    greeted += [(z > 0, {"rows": r, "cols": c - 8}), (z < 3, {"rows": r, "cols": c + 8})]
    expected = jnp.int32(4)
    for peer in group_peers + [partner]:
        pl.semaphore_signal(barrier, inc=1, device_id=peer, device_id_type=MESH)
    for ok, peer in greeted:
        expected = expected + ok.astype(jnp.int32)

        @pl.when(ok)
        def _(peer=peer):
            pl.semaphore_signal(barrier, inc=1, device_id=peer, device_id_type=MESH)

    is_left, is_right, is_top, is_bottom = c == 0, c == n_c - 1, r == 0, r == n_r - 1
    flat = lambda ref: ref.reshape(ROWS * PITCH, M)
    fu, fv, fw, fu2, f3 = flat(u), flat(v), flat(w), flat(u2), flat(t3)

    def zero_sides(f, low, high):
        zero = jnp.zeros((high + 1 - low, M), jnp.float32)

        @pl.when(is_left)
        def _():
            f[pl.ds((Y0 + low) * PITCH - 1, high + 1 - low, stride=PITCH), :] = zero

        @pl.when(is_right)
        def _():
            f[pl.ds((Y0 + low) * PITCH + NX, high + 1 - low, stride=PITCH), :] = zero

    def zero_rows(f, low, high):
        zero = jnp.zeros((PITCH, M), jnp.float32)
        for edge, row in ((is_top, -1), (is_bottom, NY)):
            if low <= row < high:

                @pl.when(edge)
                def _(row=row):
                    f[pl.ds((Y0 + row) * PITCH - 4, PITCH), :] = zero

    zero_sides(fu, -DY, NY + DY)
    zero_sides(f3, -DY, NY + DY)
    zero_rows(fu, -DY, NY + DY)
    zero_rows(f3, -DY, NY + DY)

    sent = []
    used = [0]

    def copy_to(source, target, peer):
        k = used[0]
        used[0] += 1
        return pltpu.make_async_remote_copy(
            src_ref=source, dst_ref=target, send_sem=send_sems.at[k], recv_sem=recv_sems.at[k],
            device_id=peer, device_id_type=MESH,
        )

    def halo(ref, rows, cols, dr, dc):
        (y1, y2), (x1, x2) = rows, cols
        down, aside = -dr * NY, 0
        if dc < 0:
            aside = NX
        if dc > 0:
            down, aside = down - 1, PITCH - NX
        source = ref.at[Y0 + y1 : Y0 + y2, x1:x2, :]
        target = ref.at[Y0 + y1 + down : Y0 + y2 + down, x1 + aside : x2 + aside, :]
        return exists(dr, dc), exists(-dr, -dc), copy_to(source, target, neighbour(dr, dc))

    def when(ok, do):
        if ok is None:
            do()
        else:
            pl.when(ok)(do)

    def start(items):
        for goes, _, copy in items:
            when(goes, copy.start)
            sent.append((goes, copy))

    def arrive(items):
        for _, comes, copy in items:
            when(comes, copy.wait_recv)

    def finish(count=None):
        for goes, copy in sent[:count]:
            when(goes, copy.wait_send)
        del sent[:count]

    load_t.wait()
    load_w.wait()
    pl.semaphore_wait(barrier, expected)

    def edge_cols(dc, low, high):
        return (low, high) if dc < 0 else (NX - high, NX - low)

    def row_halo(ref, low, high, dr, dc, depth=None):
        rows = (low, high) if dr < 0 else (NY - high, NY - low)
        return halo(ref, rows, edge_cols(dc, 0, depth) if dc else (0, NX), dr, dc)

    def from_row_neighbour(dr):
        out = [row_halo(u, 0, 3, dr, 0), row_halo(w, 0, 2, dr, 0)]
        for dc in (-1, 1):
            out.append(row_halo(u, 0, 3, dr, dc, 3))
            out.append(row_halo(w, 0, 2, dr, dc, 2))
        return out

    def again_from_row_neighbour(dr):
        return [row_halo(t3, 0, 3, dr, dc, 3) for dc in (0, -1, 1)]

    from_below = from_row_neighbour(-1)
    from_above = from_row_neighbour(1)
    first = []
    for j in range(CHUNKS):
        rows = (MAIN[j], MAIN[j + 1])
        first.append(
            [halo(u, rows, edge_cols(dc, 0, 3), 0, dc) for dc in (-1, 1)]
            + [halo(w, rows, edge_cols(dc, 0, 2), 0, dc) for dc in (-1, 1)]
        )
    start(from_above)
    start(from_below)
    start(first[0])
    for items in first[1:]:
        start(items)
    first_sends = len(sent)


    def chain_stage(k):
        if k > 0:

            @pl.when(z < 3)
            def _():
                pl.semaphore_wait(chain.at[k - 1], 1)

        if k < 3:

            @pl.when(z > 0)
            def _():
                pl.semaphore_signal(chain.at[k], inc=1, device_id={"rows": r, "cols": c - 8}, device_id_type=MESH)

    chain_stage(0)

    def step(src, low, high, tiles, store, first=False, last=False):
        def body(i, carry):
            north, centre = carry
            base = pl.multiple_of((Y0 + low + i) * PITCH, 8)
            south, new = [], []
            for k in range(tiles):
                at = base + 8 * k
                s = src[pl.ds(pl.multiple_of(at + PITCH, 8), 8), :]
                left = src[pl.ds(at - 1, 8), :]
                right = src[pl.ds(at + 1, 8), :]
                cr = fw[pl.ds(pl.multiple_of(at, 8), 8), :]
                spread = (left + right) + (north[k] + s)
                taken = centre[k] * cr
                if first:
                    taken = taken + taken
                grown = spread + centre[k] * (8.0 - taken)
                new.append(grown * (0.2 if first else 0.05 if last else 0.1))
                south.append(s)
            store(low + i, base, new)
            return tuple(centre), tuple(south)

        at = (Y0 + low - 1) * PITCH
        north = tuple(src[pl.ds(at + 8 * k, 8), :] for k in range(tiles))
        centre = tuple(src[pl.ds(at + PITCH + 8 * k, 8), :] for k in range(tiles))
        lax.fori_loop(0, high - low, body, (north, centre), unroll=2)

    def store_to(dst):
        def store(row, base, new):
            for k, value in enumerate(new):
                dst[pl.ds(pl.multiple_of(base + 8 * k, 8), 8), :] = value

        return store

    def rows_at(ends, j, s):
        if j == CAP:
            return s - ends[CHUNKS - 1] + NY, s
        return (ends[j - 1] - s if j else s), ends[j] - s

    place = lax.broadcasted_iota(jnp.int32, (8, M), 0)

    second = []
    for j in range(CHUNKS + 1):
        if j == CAP:
            arrive(from_above)
        else:
            arrive(first[j])
        if j == CHUNKS - 1:
            arrive(from_below)
        low, high = rows_at(A_ENDS, j, 1)
        step(fu, low, high, 5, store_to(fv), first=True)
        zero_sides(fv, low, high)
        zero_rows(fv, low, high)
        low, high = rows_at(A_ENDS, j, 2)
        step(fv, low, high, 5, store_to(fu2))
        zero_sides(fu2, low, high)
        zero_rows(fu2, low, high)
        low, high = rows_at(A_ENDS, j, 3)
        step(fu2, low, high, 4, store_to(f3))
        items = [halo(t3, (low, high), edge_cols(dc, 0, 3), 0, dc) for dc in (-1, 1)]
        start(items)
        second.append(items)
        if j == CHUNKS - 1:
            again_from_above = again_from_row_neighbour(1)
            start(again_from_above)
        if j == CAP:
            again_from_below = again_from_row_neighbour(-1)
            start(again_from_below)
        if j in (0, 2):
            chain_stage(1 + j // 2)
    finish(first_sends)


    def store_end(row, base, new, first_row):
        for k, value in enumerate(new):
            end[row, 8 * k : 8 * k + 8, :] = value
        total = (new[0] + new[1]) + (new[2] + new[3])
        tot[pl.ds(row - DY if first_row >= DY else row + NY - DY, 1), :] = jnp.sum(total, axis=0, keepdims=True)

    def running(i, _):
        carry = jnp.zeros((1, M), jnp.float32)
        for k in range(4):
            value = end[i, 8 * k : 8 * k + 8, :]
            for shift in (1, 2, 4):
                value = value + jnp.where(place >= shift, pltpu.roll(value, shift, 0), 0.0)
            value = value + carry
            here[i, 8 * k : 8 * k + 8, :] = value
            carry = value[7:8, :]
        return 0

    def quarter(j):
        return pl.ds(j * QUARTER, QUARTER)

    def group_sum(j):
        arrive(totals[j])
        own = [p1[k, quarter(j), :] for k in range(4)]
        group[quarter(j), :] = (own[0] + own[1]) + (own[2] + own[3])
        items = [
            (g + k < 8, g >= k, copy_to(group.at[quarter(j), :], p2.at[g, quarter(j), :], {"rows": r, "cols": c + 4 * k}))
            for k in range(1, 8)
        ]
        start(items)
        return items

    totals, groups = [], []
    for j in range(CHUNKS + 1):
        arrive(second[j])
        if j == CHUNKS - 1:
            arrive(again_from_below)
        if j == CAP:
            arrive(again_from_above)
        low, high = rows_at(B_ENDS, j, 4)
        step(f3, low, high, 5, store_to(fv))
        zero_sides(fv, low, high)
        zero_rows(fv, low, high)
        low, high = rows_at(B_ENDS, j, 5)
        step(fv, low, high, 5, store_to(fu))
        zero_sides(fu, low, high)
        zero_rows(fu, low, high)
        low, high = rows_at(B_ENDS, j, 6)
        step(fu, low, high, 4, functools.partial(store_end, first_row=low), last=True)
        if j == CHUNKS - 1:
            continue
        k = min(j, CHUNKS - 1)
        items = [(None, None, copy_to(tot.at[quarter(k), :], p1.at[x, quarter(k), :], peer)) for peer in group_peers]
        start(items)
        totals.append(items)
        p1[x, quarter(k), :] = tot[quarter(k), :]
    chain_stage(3)
    for j in range(CHUNKS):
        groups.append(group_sum(j))
    lax.fori_loop(0, NY, running, 0, unroll=2)
    for j in range(CHUNKS):
        arrive(groups[j])
        before = jnp.zeros((QUARTER, M), jnp.float32)
        for k in range(7):
            before = before + jnp.where(k < g, p2[k, quarter(j), :], 0.0)
        for k in range(3):
            before = before + jnp.where(k < x, p1[k, quarter(j), :], 0.0)
        at = DY + j * QUARTER
        if j < CHUNKS - 1:
            below[at : at + QUARTER, :] = before
        else:
            below[at:NY, :] = before[: NY - at]
            below[0:DY, :] = before[NY - at :]
    finish()

def body(tracer, crowding):
    vmem = pl.BlockSpec(memory_space=pltpu.VMEM)
    hbm = pl.BlockSpec(memory_space=pltpu.HBM)
    f32 = jnp.float32
    dma = pltpu.SemaphoreType.DMA
    end, here, below = pl.pallas_call(
        kernel,
        out_shape=(
            jax.ShapeDtypeStruct((NY, NX, M), f32),
            jax.ShapeDtypeStruct((NY, NX, M), f32),
            jax.ShapeDtypeStruct((NY, M), f32),
        ),
        in_specs=[hbm, hbm],
        out_specs=(vmem, vmem, vmem),
        scratch_shapes=[
            pltpu.VMEM((ROWS, PITCH, M), f32),
            pltpu.VMEM((ROWS, PITCH, M), f32),
            pltpu.VMEM((ROWS, PITCH, M), f32),
            pltpu.VMEM((ROWS, PITCH, M), f32),
            pltpu.VMEM((ROWS, PITCH, M), f32),
            pltpu.VMEM((NY, M), f32),
            pltpu.VMEM((4, NY, M), f32),
            pltpu.VMEM((8, NY, M), f32),
            pltpu.VMEM((NY, M), f32),
            dma((2,)), dma((COUNT,)), dma((COUNT,)),
            pltpu.SemaphoreType.REGULAR((3,)),
        ],
        compiler_params=pltpu.CompilerParams(
            collective_id=0, has_side_effects=True, vmem_limit_bytes=50 * 1024 * 1024
        ),
    )(tracer, crowding)
    potential = (here + below[:, None, :]) * (1.0 / 1024)
    return (potential, end)


def solution(mesh):
    spec = P("rows", "cols", None)
    return jax.shard_map(body, mesh=mesh, in_specs=(spec, spec), out_specs=(spec, spec), check_vma=False)
```

```python
import functools

import jax
import jax.numpy as jnp
from jax import lax
from jax.experimental import pallas as pl
from jax.experimental.pallas import tpu as pltpu
from jax.sharding import PartitionSpec as P

NY, NX, M = 96, 32, 128
PITCH = 40
Y0 = 8
ROWS = NY + 2 * Y0
DY = 6
QUARTER = NY // 4
MESH = pl.DeviceIdType.MESH
DIRECTIONS = [(dr, dc) for dr in (-1, 0, 1) for dc in (-1, 0, 1) if (dr, dc) != (0, 0)]


CHUNKS = 4
CAP = CHUNKS
A_ENDS = (37, 61, 85, NY + 3)
B_ENDS = (36, 60, 84, NY + DY)
MAIN = (0, 38, 62, 86, NY)
COUNT = 96


def kernel(
    tracer, crowding, end, here, below,
    u, v, w, u2, t3, tot, p1, p2, group,
    in_sem, send_sems, recv_sems, chain,
):
    r = lax.axis_index("rows")
    c = lax.axis_index("cols")
    n_r, n_c = 4, 32
    x = lax.rem(c, 4)
    g = lax.div(c, 4)
    z = lax.div(g, 2)
    interior = lambda ref: ref.at[Y0 : Y0 + NY, 0:NX, :]
    load_t = pltpu.make_async_copy(tracer, interior(u), in_sem.at[0])
    load_w = pltpu.make_async_copy(crowding, interior(w), in_sem.at[1])
    load_t.start()
    load_w.start()

    def exists(dr, dc):
        ok = None
        for there in ((r > 0) if dr < 0 else (r < n_r - 1) if dr > 0 else None,
                      (c > 0) if dc < 0 else (c < n_c - 1) if dc > 0 else None):
            if there is not None:
                ok = there if ok is None else ok & there
        return ok

    def neighbour(dr, dc):
        return {"rows": r + dr, "cols": c + dc}

    barrier = pltpu.get_barrier_semaphore()
    group_peers = [{"rows": r, "cols": g * 4 + lax.rem(x + o, 4)} for o in (1, 2, 3)]
    partner = {"rows": r, "cols": (z * 2 + 1 - lax.rem(g, 2)) * 4 + x}
    greeted = [(exists(*d), neighbour(*d)) for d in DIRECTIONS]
    greeted += [(z > 0, {"rows": r, "cols": c - 8}), (z < 3, {"rows": r, "cols": c + 8})]
    expected = jnp.int32(4)
    for peer in group_peers + [partner]:
        pl.semaphore_signal(barrier, inc=1, device_id=peer, device_id_type=MESH)
    for ok, peer in greeted:
        expected = expected + ok.astype(jnp.int32)

        @pl.when(ok)
        def _(peer=peer):
            pl.semaphore_signal(barrier, inc=1, device_id=peer, device_id_type=MESH)

    is_left, is_right, is_top, is_bottom = c == 0, c == n_c - 1, r == 0, r == n_r - 1
    flat = lambda ref: ref.reshape(ROWS * PITCH, M)
    fu, fv, fw, fu2, f3 = flat(u), flat(v), flat(w), flat(u2), flat(t3)

    def zero_sides(f, low, high):
        zero = jnp.zeros((high + 1 - low, M), jnp.float32)

        @pl.when(is_left)
        def _():
            f[pl.ds((Y0 + low) * PITCH - 1, high + 1 - low, stride=PITCH), :] = zero

        @pl.when(is_right)
        def _():
            f[pl.ds((Y0 + low) * PITCH + NX, high + 1 - low, stride=PITCH), :] = zero

    def zero_rows(f, low, high):
        zero = jnp.zeros((PITCH, M), jnp.float32)
        for edge, row in ((is_top, -1), (is_bottom, NY)):
            if low <= row < high:

                @pl.when(edge)
                def _(row=row):
                    f[pl.ds((Y0 + row) * PITCH - 4, PITCH), :] = zero

    zero_sides(fu, -DY, NY + DY)
    zero_sides(f3, -DY, NY + DY)
    zero_rows(fu, -DY, NY + DY)
    zero_rows(f3, -DY, NY + DY)

    sent = []
    used = [0]

    def copy_to(source, target, peer):
        k = used[0]
        used[0] += 1
        return pltpu.make_async_remote_copy(
            src_ref=source, dst_ref=target, send_sem=send_sems.at[k], recv_sem=recv_sems.at[k],
            device_id=peer, device_id_type=MESH,
        )

    def halo(ref, rows, cols, dr, dc):
        (y1, y2), (x1, x2) = rows, cols
        down, aside = -dr * NY, 0
        if dc < 0:
            aside = NX
        if dc > 0:
            down, aside = down - 1, PITCH - NX
        source = ref.at[Y0 + y1 : Y0 + y2, x1:x2, :]
        target = ref.at[Y0 + y1 + down : Y0 + y2 + down, x1 + aside : x2 + aside, :]
        return exists(dr, dc), exists(-dr, -dc), copy_to(source, target, neighbour(dr, dc))

    def when(ok, do):
        if ok is None:
            do()
        else:
            pl.when(ok)(do)

    def start(items):
        for goes, _, copy in items:
            when(goes, copy.start)
            sent.append((goes, copy))

    def arrive(items):
        for _, comes, copy in items:
            when(comes, copy.wait_recv)

    def finish(count=None):
        for goes, copy in sent[:count]:
            when(goes, copy.wait_send)
        del sent[:count]

    load_t.wait()
    load_w.wait()
    pl.semaphore_wait(barrier, expected)

    def edge_cols(dc, low, high):
        return (low, high) if dc < 0 else (NX - high, NX - low)

    def row_halo(ref, low, high, dr, dc, depth=None):
        rows = (low, high) if dr < 0 else (NY - high, NY - low)
        return halo(ref, rows, edge_cols(dc, 0, depth) if dc else (0, NX), dr, dc)

    def from_row_neighbour(dr):
        out = [row_halo(u, 0, 3, dr, 0), row_halo(w, 0, 2, dr, 0)]
        for dc in (-1, 1):
            out.append(row_halo(u, 0, 3, dr, dc, 3))
            out.append(row_halo(w, 0, 2, dr, dc, 2))
        return out

    def again_from_row_neighbour(dr):
        return [row_halo(t3, 0, 3, dr, dc, 3) for dc in (0, -1, 1)]

    from_below = from_row_neighbour(-1)
    from_above = from_row_neighbour(1)
    first = []
    for j in range(CHUNKS):
        rows = (MAIN[j], MAIN[j + 1])
        first.append(
            [halo(u, rows, edge_cols(dc, 0, 3), 0, dc) for dc in (-1, 1)]
            + [halo(w, rows, edge_cols(dc, 0, 2), 0, dc) for dc in (-1, 1)]
        )
    start(from_above)
    start(from_below)
    start(first[0])
    for items in first[1:]:
        start(items)
    first_sends = len(sent)


    def chain_stage(k):
        if k > 0:

            @pl.when(z < 3)
            def _():
                pl.semaphore_wait(chain.at[k - 1], 1)

        if k < 3:

            @pl.when(z > 0)
            def _():
                pl.semaphore_signal(chain.at[k], inc=1, device_id={"rows": r, "cols": c - 8}, device_id_type=MESH)

    chain_stage(0)

    def step(src, low, high, tiles, store, first=False, last=False):
        def body(i, carry):
            north, centre = carry
            base = pl.multiple_of((Y0 + low + i) * PITCH, 8)
            south, new = [], []
            for k in range(tiles):
                at = base + 8 * k
                s = src[pl.ds(pl.multiple_of(at + PITCH, 8), 8), :]
                left = src[pl.ds(at - 1, 8), :]
                right = src[pl.ds(at + 1, 8), :]
                cr = fw[pl.ds(pl.multiple_of(at, 8), 8), :]
                spread = (left + right) + (north[k] + s)
                taken = centre[k] * cr
                if first:
                    taken = taken + taken
                grown = spread + centre[k] * (8.0 - taken)
                new.append(grown * (0.2 if first else 0.05 if last else 0.1))
                south.append(s)
            store(low + i, base, new)
            return tuple(centre), tuple(south)

        at = (Y0 + low - 1) * PITCH
        north = tuple(src[pl.ds(at + 8 * k, 8), :] for k in range(tiles))
        centre = tuple(src[pl.ds(at + PITCH + 8 * k, 8), :] for k in range(tiles))
        lax.fori_loop(0, high - low, body, (north, centre), unroll=2)

    def store_to(dst):
        def store(row, base, new):
            for k, value in enumerate(new):
                dst[pl.ds(pl.multiple_of(base + 8 * k, 8), 8), :] = value

        return store

    def rows_at(ends, j, s):
        if j == CAP:
            return s - ends[CHUNKS - 1] + NY, s
        return (ends[j - 1] - s if j else s), ends[j] - s

    place = lax.broadcasted_iota(jnp.int32, (8, M), 0)

    second = []
    for j in range(CHUNKS + 1):
        if j == CAP:
            arrive(from_above)
        else:
            arrive(first[j])
        if j == CHUNKS - 1:
            arrive(from_below)
        low, high = rows_at(A_ENDS, j, 1)
        step(fu, low, high, 5, store_to(fv), first=True)
        zero_sides(fv, low, high)
        zero_rows(fv, low, high)
        low, high = rows_at(A_ENDS, j, 2)
        step(fv, low, high, 5, store_to(fu2))
        zero_sides(fu2, low, high)
        zero_rows(fu2, low, high)
        low, high = rows_at(A_ENDS, j, 3)
        step(fu2, low, high, 4, store_to(f3))
        items = [halo(t3, (low, high), edge_cols(dc, 0, 3), 0, dc) for dc in (-1, 1)]
        start(items)
        second.append(items)
        if j == CHUNKS - 1:
            again_from_above = again_from_row_neighbour(1)
            start(again_from_above)
        if j == CAP:
            again_from_below = again_from_row_neighbour(-1)
            start(again_from_below)
        if j in (0, 2):
            chain_stage(1 + j // 2)
    finish(first_sends)


    def store_end(row, base, new, first_row):
        for k, value in enumerate(new):
            end[row, 8 * k : 8 * k + 8, :] = value
        total = (new[0] + new[1]) + (new[2] + new[3])
        tot[pl.ds(row - DY if first_row >= DY else row + NY - DY, 1), :] = jnp.sum(total, axis=0, keepdims=True)

    def running(i, _):
        carry = jnp.zeros((1, M), jnp.float32)
        for k in range(4):
            value = end[i, 8 * k : 8 * k + 8, :]
            for shift in (1, 2, 4):
                value = value + jnp.where(place >= shift, pltpu.roll(value, shift, 0), 0.0)
            value = value + carry
            here[i, 8 * k : 8 * k + 8, :] = value
            carry = value[7:8, :]
        return 0

    def quarter(j):
        return pl.ds(j * QUARTER, QUARTER)

    def group_sum(j):
        arrive(totals[j])
        own = [p1[k, quarter(j), :] for k in range(4)]
        group[quarter(j), :] = (own[0] + own[1]) + (own[2] + own[3])
        items = [
            (g + k < 8, g >= k, copy_to(group.at[quarter(j), :], p2.at[g, quarter(j), :], {"rows": r, "cols": c + 4 * k}))
            for k in range(1, 8)
        ]
        start(items)
        return items

    totals, groups = [], []
    for j in range(CHUNKS + 1):
        arrive(second[j])
        if j == CHUNKS - 1:
            arrive(again_from_below)
        if j == CAP:
            arrive(again_from_above)
        low, high = rows_at(B_ENDS, j, 4)
        step(f3, low, high, 5, store_to(fv))
        zero_sides(fv, low, high)
        zero_rows(fv, low, high)
        low, high = rows_at(B_ENDS, j, 5)
        step(fv, low, high, 5, store_to(fu))
        zero_sides(fu, low, high)
        zero_rows(fu, low, high)
        low, high = rows_at(B_ENDS, j, 6)
        step(fu, low, high, 4, functools.partial(store_end, first_row=low), last=True)
        if j == CHUNKS - 1:
            continue
        k = min(j, CHUNKS - 1)
        items = [(None, None, copy_to(tot.at[quarter(k), :], p1.at[x, quarter(k), :], peer)) for peer in group_peers]
        start(items)
        totals.append(items)
        p1[x, quarter(k), :] = tot[quarter(k), :]
    chain_stage(3)
    for j in range(CHUNKS):
        groups.append(group_sum(j))
    lax.fori_loop(0, NY, running, 0, unroll=2)
    for j in range(CHUNKS):
        arrive(groups[j])
        before = jnp.zeros((QUARTER, M), jnp.float32)
        for k in range(7):
            before = before + jnp.where(k < g, p2[k, quarter(j), :], 0.0)
        for k in range(3):
            before = before + jnp.where(k < x, p1[k, quarter(j), :], 0.0)
        at = DY + j * QUARTER
        if j < CHUNKS - 1:
            below[at : at + QUARTER, :] = before
        else:
            below[at:NY, :] = before[: NY - at]
            below[0:DY, :] = before[NY - at :]
    finish()

PIECES = 4


def write_out(here, below, end, potential_out, end_out, potential, sems):
    rest = pltpu.make_async_copy(end, end_out, sems.at[PIECES])
    rest.start()
    rows = NY // PIECES
    pieces = []
    for k in range(PIECES):
        part = slice(k * rows, (k + 1) * rows)

        def row(i, _):
            potential[i] = (here[i] + below[pl.ds(i, 1), :]) * (1.0 / 1024)
            return 0

        lax.fori_loop(k * rows, (k + 1) * rows, row, 0, unroll=4)
        piece = pltpu.make_async_copy(potential.at[part], potential_out.at[part], sems.at[k])
        piece.start()
        pieces.append(piece)
    for piece in pieces:
        piece.wait()
    rest.wait()


def body(tracer, crowding):
    vmem = pl.BlockSpec(memory_space=pltpu.VMEM)
    hbm = pl.BlockSpec(memory_space=pltpu.HBM)
    f32 = jnp.float32
    dma = pltpu.SemaphoreType.DMA
    end, here, below = pl.pallas_call(
        kernel,
        out_shape=(
            jax.ShapeDtypeStruct((NY, NX, M), f32),
            jax.ShapeDtypeStruct((NY, NX, M), f32),
            jax.ShapeDtypeStruct((NY, M), f32),
        ),
        in_specs=[hbm, hbm],
        out_specs=(vmem, vmem, vmem),
        scratch_shapes=[
            pltpu.VMEM((ROWS, PITCH, M), f32),
            pltpu.VMEM((ROWS, PITCH, M), f32),
            pltpu.VMEM((ROWS, PITCH, M), f32),
            pltpu.VMEM((ROWS, PITCH, M), f32),
            pltpu.VMEM((ROWS, PITCH, M), f32),
            pltpu.VMEM((NY, M), f32),
            pltpu.VMEM((4, NY, M), f32),
            pltpu.VMEM((8, NY, M), f32),
            pltpu.VMEM((NY, M), f32),
            dma((2,)), dma((COUNT,)), dma((COUNT,)),
            pltpu.SemaphoreType.REGULAR((3,)),
        ],
        compiler_params=pltpu.CompilerParams(
            collective_id=0, has_side_effects=True, vmem_limit_bytes=50 * 1024 * 1024
        ),
    )(tracer, crowding)
    potential, end = pl.pallas_call(
        write_out,
        out_shape=(jax.ShapeDtypeStruct((NY, NX, M), f32), jax.ShapeDtypeStruct((NY, NX, M), f32)),
        in_specs=[vmem, vmem, vmem],
        out_specs=(hbm, hbm),
        scratch_shapes=[pltpu.VMEM((NY, NX, M), f32), dma((PIECES + 1,))],
        compiler_params=pltpu.CompilerParams(vmem_limit_bytes=8 * 1024 * 1024),
    )(here, below, end)
    return (potential, end)


def solution(mesh):
    spec = P("rows", "cols", None)
    return jax.shard_map(body, mesh=mesh, in_specs=(spec, spec), out_specs=(spec, spec), check_vma=False)
```

```python
import functools

import jax
import jax.numpy as jnp
from jax import lax
from jax.experimental import pallas as pl
from jax.experimental.pallas import tpu as pltpu
from jax.sharding import PartitionSpec as P

NY, NX, M = 96, 32, 128
PITCH = 40
Y0 = 8
ROWS = NY + 2 * Y0
DY = 6
QUARTER = NY // 4
MESH = pl.DeviceIdType.MESH
DIRECTIONS = [(dr, dc) for dr in (-1, 0, 1) for dc in (-1, 0, 1) if (dr, dc) != (0, 0)]


CHUNKS = 4
CAP = CHUNKS
A_ENDS = (37, 61, 85, NY + 3)
B_ENDS = (36, 60, 84, NY + DY)
MAIN = (0, 38, 62, 86, NY)
COUNT = 96


def kernel(
    tracer, crowding, end, here, below,
    u, v, w, u2, t3, tot, p1, p2, group,
    in_sem, send_sems, recv_sems, chain,
):
    r = lax.axis_index("rows")
    c = lax.axis_index("cols")
    n_r, n_c = 4, 32
    x = lax.rem(c, 4)
    g = lax.div(c, 4)
    z = lax.div(g, 2)
    interior = lambda ref: ref.at[Y0 : Y0 + NY, 0:NX, :]
    load_t = pltpu.make_async_copy(tracer, interior(u), in_sem.at[0])
    load_w = pltpu.make_async_copy(crowding, interior(w), in_sem.at[1])
    load_t.start()
    load_w.start()

    def exists(dr, dc):
        ok = None
        for there in ((r > 0) if dr < 0 else (r < n_r - 1) if dr > 0 else None,
                      (c > 0) if dc < 0 else (c < n_c - 1) if dc > 0 else None):
            if there is not None:
                ok = there if ok is None else ok & there
        return ok

    def neighbour(dr, dc):
        return {"rows": r + dr, "cols": c + dc}

    barrier = pltpu.get_barrier_semaphore()
    group_peers = [{"rows": r, "cols": g * 4 + lax.rem(x + o, 4)} for o in (1, 2, 3)]
    partner = {"rows": r, "cols": (z * 2 + 1 - lax.rem(g, 2)) * 4 + x}
    greeted = [(exists(*d), neighbour(*d)) for d in DIRECTIONS]
    greeted += [(z > 0, {"rows": r, "cols": c - 8}), (z < 3, {"rows": r, "cols": c + 8})]
    expected = jnp.int32(4)
    for peer in group_peers + [partner]:
        pl.semaphore_signal(barrier, inc=1, device_id=peer, device_id_type=MESH)
    for ok, peer in greeted:
        expected = expected + ok.astype(jnp.int32)

        @pl.when(ok)
        def _(peer=peer):
            pl.semaphore_signal(barrier, inc=1, device_id=peer, device_id_type=MESH)

    is_left, is_right, is_top, is_bottom = c == 0, c == n_c - 1, r == 0, r == n_r - 1
    flat = lambda ref: ref.reshape(ROWS * PITCH, M)
    fu, fv, fw, fu2, f3 = flat(u), flat(v), flat(w), flat(u2), flat(t3)

    def zero_sides(f, low, high):
        zero = jnp.zeros((high + 1 - low, M), jnp.float32)

        @pl.when(is_left)
        def _():
            f[pl.ds((Y0 + low) * PITCH - 1, high + 1 - low, stride=PITCH), :] = zero

        @pl.when(is_right)
        def _():
            f[pl.ds((Y0 + low) * PITCH + NX, high + 1 - low, stride=PITCH), :] = zero

    def zero_rows(f, low, high):
        zero = jnp.zeros((PITCH, M), jnp.float32)
        for edge, row in ((is_top, -1), (is_bottom, NY)):
            if low <= row < high:

                @pl.when(edge)
                def _(row=row):
                    f[pl.ds((Y0 + row) * PITCH - 4, PITCH), :] = zero

    zero_sides(fu, -DY, NY + DY)
    zero_sides(f3, -DY, NY + DY)
    zero_rows(fu, -DY, NY + DY)
    zero_rows(f3, -DY, NY + DY)

    sent = []
    used = [0]

    def copy_to(source, target, peer):
        k = used[0]
        used[0] += 1
        return pltpu.make_async_remote_copy(
            src_ref=source, dst_ref=target, send_sem=send_sems.at[k], recv_sem=recv_sems.at[k],
            device_id=peer, device_id_type=MESH,
        )

    def halo(ref, rows, cols, dr, dc):
        (y1, y2), (x1, x2) = rows, cols
        down, aside = -dr * NY, 0
        if dc < 0:
            aside = NX
        if dc > 0:
            down, aside = down - 1, PITCH - NX
        source = ref.at[Y0 + y1 : Y0 + y2, x1:x2, :]
        target = ref.at[Y0 + y1 + down : Y0 + y2 + down, x1 + aside : x2 + aside, :]
        return exists(dr, dc), exists(-dr, -dc), copy_to(source, target, neighbour(dr, dc))

    def when(ok, do):
        if ok is None:
            do()
        else:
            pl.when(ok)(do)

    def start(items):
        for goes, _, copy in items:
            when(goes, copy.start)
            sent.append((goes, copy))

    def arrive(items):
        for _, comes, copy in items:
            when(comes, copy.wait_recv)

    def finish(count=None):
        for goes, copy in sent[:count]:
            when(goes, copy.wait_send)
        del sent[:count]

    load_t.wait()
    load_w.wait()
    pl.semaphore_wait(barrier, expected)

    def edge_cols(dc, low, high):
        return (low, high) if dc < 0 else (NX - high, NX - low)

    def row_halo(ref, low, high, dr, dc, depth=None):
        rows = (low, high) if dr < 0 else (NY - high, NY - low)
        return halo(ref, rows, edge_cols(dc, 0, depth) if dc else (0, NX), dr, dc)

    def from_row_neighbour(dr):
        out = [row_halo(u, 0, 3, dr, 0), row_halo(w, 0, 2, dr, 0)]
        for dc in (-1, 1):
            out.append(row_halo(u, 0, 3, dr, dc, 3))
            out.append(row_halo(w, 0, 2, dr, dc, 2))
        return out

    def again_from_row_neighbour(dr):
        return [row_halo(t3, 0, 3, dr, dc, 3) for dc in (0, -1, 1)]

    from_below = from_row_neighbour(-1)
    from_above = from_row_neighbour(1)
    first = []
    for j in range(CHUNKS):
        rows = (MAIN[j], MAIN[j + 1])
        first.append(
            [halo(u, rows, edge_cols(dc, 0, 3), 0, dc) for dc in (-1, 1)]
            + [halo(w, rows, edge_cols(dc, 0, 2), 0, dc) for dc in (-1, 1)]
        )
    start(from_above)
    start(from_below)
    start(first[0])
    for items in first[1:]:
        start(items)
    first_sends = len(sent)


    def chain_stage(k):
        if k > 0:

            @pl.when(z < 3)
            def _():
                pl.semaphore_wait(chain.at[k - 1], 1)

        if k < 3:

            @pl.when(z > 0)
            def _():
                pl.semaphore_signal(chain.at[k], inc=1, device_id={"rows": r, "cols": c - 8}, device_id_type=MESH)

    chain_stage(0)

    def step(src, low, high, tiles, store, first=False, last=False):
        def body(i, carry):
            north, centre = carry
            base = pl.multiple_of((Y0 + low + i) * PITCH, 8)
            south, new = [], []
            for k in range(tiles):
                at = base + 8 * k
                s = src[pl.ds(pl.multiple_of(at + PITCH, 8), 8), :]
                left = src[pl.ds(at - 1, 8), :]
                right = src[pl.ds(at + 1, 8), :]
                cr = fw[pl.ds(pl.multiple_of(at, 8), 8), :]
                spread = (left + right) + (north[k] + s)
                taken = centre[k] * cr
                if first:
                    taken = taken + taken
                grown = spread + centre[k] * (8.0 - taken)
                new.append(grown * (0.2 if first else 0.05 if last else 0.1))
                south.append(s)
            store(low + i, base, new)
            return tuple(centre), tuple(south)

        at = (Y0 + low - 1) * PITCH
        north = tuple(src[pl.ds(at + 8 * k, 8), :] for k in range(tiles))
        centre = tuple(src[pl.ds(at + PITCH + 8 * k, 8), :] for k in range(tiles))
        lax.fori_loop(0, high - low, body, (north, centre), unroll=4 if high - low > 8 else high - low)

    def store_to(dst):
        def store(row, base, new):
            for k, value in enumerate(new):
                dst[pl.ds(pl.multiple_of(base + 8 * k, 8), 8), :] = value

        return store

    def rows_at(ends, j, s):
        if j == CAP:
            return s - ends[CHUNKS - 1] + NY, s
        return (ends[j - 1] - s if j else s), ends[j] - s

    place = lax.broadcasted_iota(jnp.int32, (8, M), 0)

    second = []
    for j in range(CHUNKS + 1):
        if j == CAP:
            arrive(from_above)
        else:
            arrive(first[j])
        if j == CHUNKS - 1:
            arrive(from_below)
        low, high = rows_at(A_ENDS, j, 1)
        step(fu, low, high, 5, store_to(fv), first=True)
        zero_sides(fv, low, high)
        zero_rows(fv, low, high)
        low, high = rows_at(A_ENDS, j, 2)
        step(fv, low, high, 5, store_to(fu2))
        zero_sides(fu2, low, high)
        zero_rows(fu2, low, high)
        low, high = rows_at(A_ENDS, j, 3)
        step(fu2, low, high, 4, store_to(f3))
        items = [halo(t3, (low, high), edge_cols(dc, 0, 3), 0, dc) for dc in (-1, 1)]
        start(items)
        second.append(items)
        if j == CHUNKS - 1:
            again_from_above = again_from_row_neighbour(1)
            start(again_from_above)
        if j == CAP:
            again_from_below = again_from_row_neighbour(-1)
            start(again_from_below)
        if j in (0, 2):
            chain_stage(1 + j // 2)
    finish(first_sends)


    def store_end(row, base, new, first_row):
        for k, value in enumerate(new):
            end[row, 8 * k : 8 * k + 8, :] = value
        total = (new[0] + new[1]) + (new[2] + new[3])
        tot[pl.ds(row - DY if first_row >= DY else row + NY - DY, 1), :] = jnp.sum(total, axis=0, keepdims=True)

    def running(i, _):
        carry = jnp.zeros((1, M), jnp.float32)
        for k in range(4):
            value = end[i, 8 * k : 8 * k + 8, :]
            for shift in (1, 2, 4):
                value = value + jnp.where(place >= shift, pltpu.roll(value, shift, 0), 0.0)
            value = value + carry
            here[i, 8 * k : 8 * k + 8, :] = value
            carry = value[7:8, :]
        return 0

    def quarter(j):
        return pl.ds(j * QUARTER, QUARTER)

    def group_sum(j):
        arrive(totals[j])
        own = [p1[k, quarter(j), :] for k in range(4)]
        group[quarter(j), :] = (own[0] + own[1]) + (own[2] + own[3])
        items = [
            (g + k < 8, g >= k, copy_to(group.at[quarter(j), :], p2.at[g, quarter(j), :], {"rows": r, "cols": c + 4 * k}))
            for k in range(1, 8)
        ]
        start(items)
        return items

    totals, groups = [], []
    for j in range(CHUNKS + 1):
        arrive(second[j])
        if j == CHUNKS - 1:
            arrive(again_from_below)
        if j == CAP:
            arrive(again_from_above)
        low, high = rows_at(B_ENDS, j, 4)
        step(f3, low, high, 5, store_to(fv))
        zero_sides(fv, low, high)
        zero_rows(fv, low, high)
        low, high = rows_at(B_ENDS, j, 5)
        step(fv, low, high, 5, store_to(fu))
        zero_sides(fu, low, high)
        zero_rows(fu, low, high)
        low, high = rows_at(B_ENDS, j, 6)
        step(fu, low, high, 4, functools.partial(store_end, first_row=low), last=True)
        if j == CHUNKS - 1:
            continue
        k = min(j, CHUNKS - 1)
        items = [(None, None, copy_to(tot.at[quarter(k), :], p1.at[x, quarter(k), :], peer)) for peer in group_peers]
        start(items)
        totals.append(items)
        p1[x, quarter(k), :] = tot[quarter(k), :]
    chain_stage(3)
    for j in range(CHUNKS):
        groups.append(group_sum(j))
    lax.fori_loop(0, NY, running, 0, unroll=2)
    for j in range(CHUNKS):
        arrive(groups[j])
        before = jnp.zeros((QUARTER, M), jnp.float32)
        for k in range(7):
            before = before + jnp.where(k < g, p2[k, quarter(j), :], 0.0)
        for k in range(3):
            before = before + jnp.where(k < x, p1[k, quarter(j), :], 0.0)
        at = DY + j * QUARTER
        if j < CHUNKS - 1:
            below[at : at + QUARTER, :] = before
        else:
            below[at:NY, :] = before[: NY - at]
            below[0:DY, :] = before[NY - at :]
    finish()

PIECES = 4


def write_out(here, below, end, potential_out, end_out, potential, sems):
    rest = pltpu.make_async_copy(end, end_out, sems.at[PIECES])
    rest.start()
    rows = NY // PIECES
    pieces = []
    for k in range(PIECES):
        part = slice(k * rows, (k + 1) * rows)

        def row(i, _):
            potential[i] = (here[i] + below[pl.ds(i, 1), :]) * (1.0 / 1024)
            return 0

        lax.fori_loop(k * rows, (k + 1) * rows, row, 0, unroll=4)
        piece = pltpu.make_async_copy(potential.at[part], potential_out.at[part], sems.at[k])
        piece.start()
        pieces.append(piece)
    for piece in pieces:
        piece.wait()
    rest.wait()


def body(tracer, crowding):
    vmem = pl.BlockSpec(memory_space=pltpu.VMEM)
    hbm = pl.BlockSpec(memory_space=pltpu.HBM)
    f32 = jnp.float32
    dma = pltpu.SemaphoreType.DMA
    end, here, below = pl.pallas_call(
        kernel,
        out_shape=(
            jax.ShapeDtypeStruct((NY, NX, M), f32),
            jax.ShapeDtypeStruct((NY, NX, M), f32),
            jax.ShapeDtypeStruct((NY, M), f32),
        ),
        in_specs=[hbm, hbm],
        out_specs=(vmem, vmem, vmem),
        scratch_shapes=[
            pltpu.VMEM((ROWS, PITCH, M), f32),
            pltpu.VMEM((ROWS, PITCH, M), f32),
            pltpu.VMEM((ROWS, PITCH, M), f32),
            pltpu.VMEM((ROWS, PITCH, M), f32),
            pltpu.VMEM((ROWS, PITCH, M), f32),
            pltpu.VMEM((NY, M), f32),
            pltpu.VMEM((4, NY, M), f32),
            pltpu.VMEM((8, NY, M), f32),
            pltpu.VMEM((NY, M), f32),
            dma((2,)), dma((COUNT,)), dma((COUNT,)),
            pltpu.SemaphoreType.REGULAR((3,)),
        ],
        compiler_params=pltpu.CompilerParams(
            collective_id=0, has_side_effects=True, vmem_limit_bytes=50 * 1024 * 1024
        ),
    )(tracer, crowding)
    potential, end = pl.pallas_call(
        write_out,
        out_shape=(jax.ShapeDtypeStruct((NY, NX, M), f32), jax.ShapeDtypeStruct((NY, NX, M), f32)),
        in_specs=[vmem, vmem, vmem],
        out_specs=(hbm, hbm),
        scratch_shapes=[pltpu.VMEM((NY, NX, M), f32), dma((PIECES + 1,))],
        compiler_params=pltpu.CompilerParams(vmem_limit_bytes=8 * 1024 * 1024),
    )(here, below, end)
    return (potential, end)


def solution(mesh):
    spec = P("rows", "cols", None)
    return jax.shard_map(body, mesh=mesh, in_specs=(spec, spec), out_specs=(spec, spec), check_vma=False)
```

```python
import functools

import jax
import jax.numpy as jnp
from jax import lax
from jax.experimental import pallas as pl
from jax.experimental.pallas import tpu as pltpu
from jax.sharding import PartitionSpec as P

NY, NX, M = 96, 32, 128
PITCH = 40
Y0 = 8
ROWS = NY + 2 * Y0
DY = 6
QUARTER = NY // 4
MESH = pl.DeviceIdType.MESH
DIRECTIONS = [(dr, dc) for dr in (-1, 0, 1) for dc in (-1, 0, 1) if (dr, dc) != (0, 0)]


CHUNKS = 4
CAP = CHUNKS
A_ENDS = (37, 61, 85, NY + 3)
B_ENDS = (36, 60, 84, NY + DY)
MAIN = (0, 38, 62, 86, NY)
COUNT = 96


def kernel(
    tracer, crowding, end, here, below,
    u, v, w, u2, t3, tot, p1, p2, group,
    in_sem, send_sems, recv_sems, chain,
):
    r = lax.axis_index("rows")
    c = lax.axis_index("cols")
    n_r, n_c = 4, 32
    x = lax.rem(c, 4)
    g = lax.div(c, 4)
    z = lax.div(g, 2)
    interior = lambda ref: ref.at[Y0 : Y0 + NY, 0:NX, :]
    load_t = pltpu.make_async_copy(tracer, interior(u), in_sem.at[0])
    load_w = pltpu.make_async_copy(crowding, interior(w), in_sem.at[1])
    load_t.start()
    load_w.start()

    def exists(dr, dc):
        ok = None
        for there in ((r > 0) if dr < 0 else (r < n_r - 1) if dr > 0 else None,
                      (c > 0) if dc < 0 else (c < n_c - 1) if dc > 0 else None):
            if there is not None:
                ok = there if ok is None else ok & there
        return ok

    def neighbour(dr, dc):
        return {"rows": r + dr, "cols": c + dc}

    barrier = pltpu.get_barrier_semaphore()
    group_peers = [{"rows": r, "cols": g * 4 + lax.rem(x + o, 4)} for o in (1, 2, 3)]
    partner = {"rows": r, "cols": (z * 2 + 1 - lax.rem(g, 2)) * 4 + x}
    greeted = [(exists(*d), neighbour(*d)) for d in DIRECTIONS]
    greeted += [(z > 0, {"rows": r, "cols": c - 8}), (z < 3, {"rows": r, "cols": c + 8})]
    expected = jnp.int32(4)
    for peer in group_peers + [partner]:
        pl.semaphore_signal(barrier, inc=1, device_id=peer, device_id_type=MESH)
    for ok, peer in greeted:
        expected = expected + ok.astype(jnp.int32)

        @pl.when(ok)
        def _(peer=peer):
            pl.semaphore_signal(barrier, inc=1, device_id=peer, device_id_type=MESH)

    is_left, is_right, is_top, is_bottom = c == 0, c == n_c - 1, r == 0, r == n_r - 1
    flat = lambda ref: ref.reshape(ROWS * PITCH, M)
    fu, fv, fw, fu2, f3 = flat(u), flat(v), flat(w), flat(u2), flat(t3)

    def zero_sides(f, low, high):
        zero = jnp.zeros((high + 1 - low, M), jnp.float32)

        @pl.when(is_left)
        def _():
            f[pl.ds((Y0 + low) * PITCH - 1, high + 1 - low, stride=PITCH), :] = zero

        @pl.when(is_right)
        def _():
            f[pl.ds((Y0 + low) * PITCH + NX, high + 1 - low, stride=PITCH), :] = zero

    def zero_rows(f, low, high):
        zero = jnp.zeros((PITCH, M), jnp.float32)
        for edge, row in ((is_top, -1), (is_bottom, NY)):
            if low <= row < high:

                @pl.when(edge)
                def _(row=row):
                    f[pl.ds((Y0 + row) * PITCH - 4, PITCH), :] = zero

    zero_sides(fu, -4, NY + 3)
    zero_sides(f3, -4, NY + 3)
    zero_rows(fu, -DY, NY + DY)
    zero_rows(f3, -DY, NY + DY)

    sent = []
    used = [0]

    def copy_to(source, target, peer):
        k = used[0]
        used[0] += 1
        return pltpu.make_async_remote_copy(
            src_ref=source, dst_ref=target, send_sem=send_sems.at[k], recv_sem=recv_sems.at[k],
            device_id=peer, device_id_type=MESH,
        )

    def halo(ref, rows, cols, dr, dc):
        (y1, y2), (x1, x2) = rows, cols
        down, aside = -dr * NY, 0
        if dc < 0:
            aside = NX
        if dc > 0:
            down, aside = down - 1, PITCH - NX
        source = ref.at[Y0 + y1 : Y0 + y2, x1:x2, :]
        target = ref.at[Y0 + y1 + down : Y0 + y2 + down, x1 + aside : x2 + aside, :]
        return exists(dr, dc), exists(-dr, -dc), copy_to(source, target, neighbour(dr, dc))

    def when(ok, do):
        if ok is None:
            do()
        else:
            pl.when(ok)(do)

    def start(items):
        for goes, _, copy in items:
            when(goes, copy.start)
            sent.append((goes, copy))

    def arrive(items):
        for _, comes, copy in items:
            when(comes, copy.wait_recv)

    def finish(count=None):
        for goes, copy in sent[:count]:
            when(goes, copy.wait_send)
        del sent[:count]

    load_t.wait()
    load_w.wait()
    pl.semaphore_wait(barrier, expected)

    def edge_cols(dc, low, high):
        return (low, high) if dc < 0 else (NX - high, NX - low)

    def row_halo(ref, low, high, dr, dc, depth=None):
        rows = (low, high) if dr < 0 else (NY - high, NY - low)
        return halo(ref, rows, edge_cols(dc, 0, depth) if dc else (0, NX), dr, dc)

    def from_row_neighbour(dr):
        out = [row_halo(u, 0, 3, dr, 0), row_halo(w, 0, 2, dr, 0)]
        for dc in (-1, 1):
            out.append(row_halo(u, 0, 3, dr, dc, 3))
            out.append(row_halo(w, 0, 2, dr, dc, 2))
        return out

    def again_from_row_neighbour(dr):
        return [row_halo(t3, 0, 3, dr, dc, 3) for dc in (0, -1, 1)]

    from_below = from_row_neighbour(-1)
    from_above = from_row_neighbour(1)
    first = []
    for j in range(CHUNKS):
        rows = (MAIN[j], MAIN[j + 1])
        first.append(
            [halo(u, rows, edge_cols(dc, 0, 3), 0, dc) for dc in (-1, 1)]
            + [halo(w, rows, edge_cols(dc, 0, 2), 0, dc) for dc in (-1, 1)]
        )
    start(from_above)
    start(from_below)
    start(first[0])
    for items in first[1:]:
        start(items)
    first_sends = len(sent)


    def chain_stage(k):
        if k > 0:

            @pl.when(z < 3)
            def _():
                pl.semaphore_wait(chain.at[k - 1], 1)

        if k < 3:

            @pl.when(z > 0)
            def _():
                pl.semaphore_signal(chain.at[k], inc=1, device_id={"rows": r, "cols": c - 8}, device_id_type=MESH)

    chain_stage(0)

    def step(src, low, high, tiles, store, first=False, last=False):
        def body(i, carry):
            north, centre = carry
            base = pl.multiple_of((Y0 + low + i) * PITCH, 8)
            south, new = [], []
            for k in range(tiles):
                at = base + 8 * k
                s = src[pl.ds(pl.multiple_of(at + PITCH, 8), 8), :]
                left = src[pl.ds(at - 1, 8), :]
                right = src[pl.ds(at + 1, 8), :]
                cr = fw[pl.ds(pl.multiple_of(at, 8), 8), :]
                spread = (left + right) + (north[k] + s)
                taken = centre[k] * cr
                if first:
                    taken = taken + taken
                grown = spread + centre[k] * (8.0 - taken)
                new.append(grown * (0.2 if first else 0.05 if last else 0.1))
                south.append(s)
            store(low + i, base, new)
            return tuple(centre), tuple(south)

        at = (Y0 + low - 1) * PITCH
        north = tuple(src[pl.ds(at + 8 * k, 8), :] for k in range(tiles))
        centre = tuple(src[pl.ds(at + PITCH + 8 * k, 8), :] for k in range(tiles))
        lax.fori_loop(0, high - low, body, (north, centre), unroll=4 if high - low > 8 else high - low)

    def store_to(dst):
        def store(row, base, new):
            for k, value in enumerate(new):
                dst[pl.ds(pl.multiple_of(base + 8 * k, 8), 8), :] = value

        return store

    def rows_at(ends, j, s):
        if j == CAP:
            return s - ends[CHUNKS - 1] + NY, s
        return (ends[j - 1] - s if j else s), ends[j] - s

    place = lax.broadcasted_iota(jnp.int32, (8, M), 0)

    second = []
    for j in range(CHUNKS + 1):
        if j == CAP:
            arrive(from_above)
        else:
            arrive(first[j])
        if j == CHUNKS - 1:
            arrive(from_below)
        low, high = rows_at(A_ENDS, j, 1)
        step(fu, low, high, 5, store_to(fv), first=True)
        zero_sides(fv, low, high)
        zero_rows(fv, low, high)
        low, high = rows_at(A_ENDS, j, 2)
        step(fv, low, high, 5, store_to(fu2))
        zero_sides(fu2, low, high)
        zero_rows(fu2, low, high)
        low, high = rows_at(A_ENDS, j, 3)
        step(fu2, low, high, 4, store_to(f3))
        items = [halo(t3, (low, high), edge_cols(dc, 0, 3), 0, dc) for dc in (-1, 1)]
        start(items)
        second.append(items)
        if j == CHUNKS - 1:
            again_from_above = again_from_row_neighbour(1)
            start(again_from_above)
        if j == CAP:
            again_from_below = again_from_row_neighbour(-1)
            start(again_from_below)
        if j in (0, 2):
            chain_stage(1 + j // 2)
    finish(first_sends)


    def store_end(row, base, new, first_row):
        for k, value in enumerate(new):
            end[row, 8 * k : 8 * k + 8, :] = value
        total = (new[0] + new[1]) + (new[2] + new[3])
        tot[pl.ds(row - DY if first_row >= DY else row + NY - DY, 1), :] = jnp.sum(total, axis=0, keepdims=True)

    def running(i, _):
        carry = jnp.zeros((1, M), jnp.float32)
        for k in range(4):
            value = end[i, 8 * k : 8 * k + 8, :]
            for shift in (1, 2, 4):
                value = value + jnp.where(place >= shift, pltpu.roll(value, shift, 0), 0.0)
            value = value + carry
            here[i, 8 * k : 8 * k + 8, :] = value
            carry = value[7:8, :]
        return 0

    def quarter(j):
        return pl.ds(j * QUARTER, QUARTER)

    def group_sum(j):
        arrive(totals[j])
        own = [p1[k, quarter(j), :] for k in range(4)]
        group[quarter(j), :] = (own[0] + own[1]) + (own[2] + own[3])
        items = [
            (g + k < 8, g >= k, copy_to(group.at[quarter(j), :], p2.at[g, quarter(j), :], {"rows": r, "cols": c + 4 * k}))
            for k in range(1, 8)
        ]
        start(items)
        return items

    totals, groups = [], []
    for j in range(CHUNKS + 1):
        arrive(second[j])
        if j == CHUNKS - 1:
            arrive(again_from_below)
        if j == CAP:
            arrive(again_from_above)
        low, high = rows_at(B_ENDS, j, 4)
        step(f3, low, high, 5, store_to(fv))
        zero_sides(fv, low, high)
        zero_rows(fv, low, high)
        low, high = rows_at(B_ENDS, j, 5)
        step(fv, low, high, 5, store_to(fu))
        zero_sides(fu, low, high)
        zero_rows(fu, low, high)
        low, high = rows_at(B_ENDS, j, 6)
        step(fu, low, high, 4, functools.partial(store_end, first_row=low), last=True)
        if j == CHUNKS - 1:
            continue
        k = min(j, CHUNKS - 1)
        items = [(None, None, copy_to(tot.at[quarter(k), :], p1.at[x, quarter(k), :], peer)) for peer in group_peers]
        start(items)
        totals.append(items)
        p1[x, quarter(k), :] = tot[quarter(k), :]
    chain_stage(3)
    for j in range(CHUNKS):
        groups.append(group_sum(j))
    lax.fori_loop(0, NY, running, 0, unroll=2)
    for j in range(CHUNKS):
        arrive(groups[j])
        before = jnp.zeros((QUARTER, M), jnp.float32)
        for k in range(7):
            before = before + jnp.where(k < g, p2[k, quarter(j), :], 0.0)
        for k in range(3):
            before = before + jnp.where(k < x, p1[k, quarter(j), :], 0.0)
        at = DY + j * QUARTER
        if j < CHUNKS - 1:
            below[at : at + QUARTER, :] = before
        else:
            below[at:NY, :] = before[: NY - at]
            below[0:DY, :] = before[NY - at :]
    finish()

PIECES = 4


def write_out(here, below, end, potential_out, end_out, potential, sems):
    rest = pltpu.make_async_copy(end, end_out, sems.at[PIECES])
    rest.start()
    rows = NY // PIECES
    pieces = []
    for k in range(PIECES):
        part = slice(k * rows, (k + 1) * rows)

        def row(i, _):
            potential[i] = (here[i] + below[pl.ds(i, 1), :]) * (1.0 / 1024)
            return 0

        lax.fori_loop(k * rows, (k + 1) * rows, row, 0, unroll=4)
        piece = pltpu.make_async_copy(potential.at[part], potential_out.at[part], sems.at[k])
        piece.start()
        pieces.append(piece)
    for piece in pieces:
        piece.wait()
    rest.wait()


def body(tracer, crowding):
    vmem = pl.BlockSpec(memory_space=pltpu.VMEM)
    hbm = pl.BlockSpec(memory_space=pltpu.HBM)
    f32 = jnp.float32
    dma = pltpu.SemaphoreType.DMA
    end, here, below = pl.pallas_call(
        kernel,
        out_shape=(
            jax.ShapeDtypeStruct((NY, NX, M), f32),
            jax.ShapeDtypeStruct((NY, NX, M), f32),
            jax.ShapeDtypeStruct((NY + 8, M), f32),
        ),
        in_specs=[hbm, hbm],
        out_specs=(vmem, vmem, vmem),
        scratch_shapes=[
            pltpu.VMEM((ROWS, PITCH, M), f32),
            pltpu.VMEM((ROWS, PITCH, M), f32),
            pltpu.VMEM((ROWS, PITCH, M), f32),
            pltpu.VMEM((ROWS, PITCH, M), f32),
            pltpu.VMEM((ROWS, PITCH, M), f32),
            pltpu.VMEM((NY + 8, M), f32),
            pltpu.VMEM((4, NY, M), f32),
            pltpu.VMEM((8, NY, M), f32),
            pltpu.VMEM((NY, M), f32),
            dma((2,)), dma((COUNT,)), dma((COUNT,)),
            pltpu.SemaphoreType.REGULAR((3,)),
        ],
        compiler_params=pltpu.CompilerParams(
            collective_id=0, has_side_effects=True, vmem_limit_bytes=50 * 1024 * 1024
        ),
    )(tracer, crowding)
    potential, end = pl.pallas_call(
        write_out,
        out_shape=(jax.ShapeDtypeStruct((NY, NX, M), f32), jax.ShapeDtypeStruct((NY, NX, M), f32)),
        in_specs=[vmem, vmem, vmem],
        out_specs=(hbm, hbm),
        scratch_shapes=[pltpu.VMEM((NY, NX, M), f32), dma((PIECES + 1,))],
        compiler_params=pltpu.CompilerParams(vmem_limit_bytes=8 * 1024 * 1024),
    )(here, below, end)
    return (potential, end)


def solution(mesh):
    spec = P("rows", "cols", None)
    return jax.shard_map(body, mesh=mesh, in_specs=(spec, spec), out_specs=(spec, spec), check_vma=False)
```

```python
import functools

import jax
import jax.numpy as jnp
from jax import lax
from jax.experimental import pallas as pl
from jax.experimental.pallas import tpu as pltpu
from jax.sharding import PartitionSpec as P

NY, NX, M = 96, 32, 128
PITCH = 40
Y0 = 8
ROWS = NY + 2 * Y0
DY = 6
QUARTER = NY // 4
MESH = pl.DeviceIdType.MESH
DIRECTIONS = [(dr, dc) for dr in (-1, 0, 1) for dc in (-1, 0, 1) if (dr, dc) != (0, 0)]


CHUNKS = 4
CAP = CHUNKS
A_ENDS = (37, 61, 85, NY + 3)
B_ENDS = (36, 60, 84, NY + DY)
MAIN = (0, 38, 62, 86, NY)
COUNT = 96


def kernel(
    tracer, crowding, end, here, below,
    u, v, w, u2, t3, tot, p1, p2, group,
    in_sem, send_sems, recv_sems, chain,
):
    r = lax.axis_index("rows")
    c = lax.axis_index("cols")
    n_r, n_c = 4, 32
    x = lax.rem(c, 4)
    g = lax.div(c, 4)
    z = lax.div(g, 2)
    interior = lambda ref: ref.at[Y0 : Y0 + NY, 0:NX, :]
    load_t = pltpu.make_async_copy(tracer, interior(u), in_sem.at[0])
    load_w = pltpu.make_async_copy(crowding, interior(w), in_sem.at[1])
    load_t.start()
    load_w.start()

    def exists(dr, dc):
        ok = None
        for there in ((r > 0) if dr < 0 else (r < n_r - 1) if dr > 0 else None,
                      (c > 0) if dc < 0 else (c < n_c - 1) if dc > 0 else None):
            if there is not None:
                ok = there if ok is None else ok & there
        return ok

    def neighbour(dr, dc):
        return {"rows": r + dr, "cols": c + dc}

    barrier = pltpu.get_barrier_semaphore()
    group_peers = [{"rows": r, "cols": g * 4 + lax.rem(x + o, 4)} for o in (1, 2, 3)]
    partner = {"rows": r, "cols": (z * 2 + 1 - lax.rem(g, 2)) * 4 + x}
    greeted = [(exists(*d), neighbour(*d)) for d in DIRECTIONS]
    greeted += [(z > 0, {"rows": r, "cols": c - 8}), (z < 3, {"rows": r, "cols": c + 8})]
    expected = jnp.int32(4)
    for peer in group_peers + [partner]:
        pl.semaphore_signal(barrier, inc=1, device_id=peer, device_id_type=MESH)
    for ok, peer in greeted:
        expected = expected + ok.astype(jnp.int32)

        @pl.when(ok)
        def _(peer=peer):
            pl.semaphore_signal(barrier, inc=1, device_id=peer, device_id_type=MESH)

    is_left, is_right, is_top, is_bottom = c == 0, c == n_c - 1, r == 0, r == n_r - 1
    flat = lambda ref: ref.reshape(ROWS * PITCH, M)
    fu, fv, fw, fu2, f3 = flat(u), flat(v), flat(w), flat(u2), flat(t3)

    def zero_sides(f, low, high):
        zero = jnp.zeros((high + 1 - low, M), jnp.float32)

        @pl.when(is_left)
        def _():
            f[pl.ds((Y0 + low) * PITCH - 1, high + 1 - low, stride=PITCH), :] = zero

        @pl.when(is_right)
        def _():
            f[pl.ds((Y0 + low) * PITCH + NX, high + 1 - low, stride=PITCH), :] = zero

    def zero_rows(f, low, high):
        zero = jnp.zeros((PITCH, M), jnp.float32)
        for edge, row in ((is_top, -1), (is_bottom, NY)):
            if low <= row < high:

                @pl.when(edge)
                def _(row=row):
                    f[pl.ds((Y0 + row) * PITCH - 4, PITCH), :] = zero

    zero_sides(fu, -4, NY + 3)
    zero_sides(f3, -4, NY + 3)
    zero_rows(fu, -DY, NY + DY)
    zero_rows(f3, -DY, NY + DY)

    sent = []
    used = [0]

    def copy_to(source, target, peer):
        k = used[0]
        used[0] += 1
        return pltpu.make_async_remote_copy(
            src_ref=source, dst_ref=target, send_sem=send_sems.at[k], recv_sem=recv_sems.at[k],
            device_id=peer, device_id_type=MESH,
        )

    def halo(ref, rows, cols, dr, dc):
        (y1, y2), (x1, x2) = rows, cols
        down, aside = -dr * NY, 0
        if dc < 0:
            aside = NX
        if dc > 0:
            down, aside = down - 1, PITCH - NX
        source = ref.at[Y0 + y1 : Y0 + y2, x1:x2, :]
        target = ref.at[Y0 + y1 + down : Y0 + y2 + down, x1 + aside : x2 + aside, :]
        return exists(dr, dc), exists(-dr, -dc), copy_to(source, target, neighbour(dr, dc))

    def when(ok, do):
        if ok is None:
            do()
        else:
            pl.when(ok)(do)

    def start(items):
        for goes, _, copy in items:
            when(goes, copy.start)
            sent.append((goes, copy))

    def arrive(items):
        for _, comes, copy in items:
            when(comes, copy.wait_recv)

    def finish(count=None):
        for goes, copy in sent[:count]:
            when(goes, copy.wait_send)
        del sent[:count]

    load_t.wait()
    load_w.wait()
    pl.semaphore_wait(barrier, expected)

    def edge_cols(dc, low, high):
        return (low, high) if dc < 0 else (NX - high, NX - low)

    def row_halo(ref, low, high, dr, dc, depth=None):
        rows = (low, high) if dr < 0 else (NY - high, NY - low)
        return halo(ref, rows, edge_cols(dc, 0, depth) if dc else (0, NX), dr, dc)

    def from_row_neighbour(dr):
        out = [row_halo(u, 0, 3, dr, 0), row_halo(w, 0, 2, dr, 0)]
        for dc in (-1, 1):
            out.append(row_halo(u, 0, 3, dr, dc, 3))
            out.append(row_halo(w, 0, 2, dr, dc, 2))
        return out

    def again_from_row_neighbour(dr):
        return [row_halo(t3, 0, 3, dr, dc, 3) for dc in (0, -1, 1)]

    from_below = from_row_neighbour(-1)
    from_above = from_row_neighbour(1)
    first = []
    for j in range(CHUNKS):
        rows = (MAIN[j], MAIN[j + 1])
        first.append(
            [halo(u, rows, edge_cols(dc, 0, 3), 0, dc) for dc in (-1, 1)]
            + [halo(w, rows, edge_cols(dc, 0, 2), 0, dc) for dc in (-1, 1)]
        )
    start(from_above)
    start(from_below)
    start(first[0])
    for items in first[1:]:
        start(items)
    first_sends = len(sent)


    def chain_stage(k):
        if k > 0:

            @pl.when(z < 3)
            def _():
                pl.semaphore_wait(chain.at[k - 1], 1)

        if k < 3:

            @pl.when(z > 0)
            def _():
                pl.semaphore_signal(chain.at[k], inc=1, device_id={"rows": r, "cols": c - 8}, device_id_type=MESH)

    chain_stage(0)

    def step(src, low, high, tiles, store, first=False, last=False):
        def body(i, carry):
            north, centre = carry
            base = pl.multiple_of((Y0 + low + i) * PITCH, 8)
            south, new = [], []
            for k in range(tiles):
                at = base + 8 * k
                s = src[pl.ds(pl.multiple_of(at + PITCH, 8), 8), :]
                left = src[pl.ds(at - 1, 8), :]
                right = src[pl.ds(at + 1, 8), :]
                cr = fw[pl.ds(pl.multiple_of(at, 8), 8), :]
                spread = (left + right) + (north[k] + s)
                taken = centre[k] * cr
                if first:
                    taken = taken + taken
                grown = spread + centre[k] * (8.0 - taken)
                new.append(grown * (0.2 if first else 0.05 if last else 0.1))
                south.append(s)
            store(low + i, base, new)
            return tuple(centre), tuple(south)

        at = (Y0 + low - 1) * PITCH
        north = tuple(src[pl.ds(at + 8 * k, 8), :] for k in range(tiles))
        centre = tuple(src[pl.ds(at + PITCH + 8 * k, 8), :] for k in range(tiles))
        lax.fori_loop(0, high - low, body, (north, centre), unroll=6 if high - low > 14 else high - low)

    def store_to(dst):
        def store(row, base, new):
            for k, value in enumerate(new):
                dst[pl.ds(pl.multiple_of(base + 8 * k, 8), 8), :] = value

        return store

    def rows_at(ends, j, s):
        if j == CAP:
            return s - ends[CHUNKS - 1] + NY, s
        return (ends[j - 1] - s if j else s), ends[j] - s

    place = lax.broadcasted_iota(jnp.int32, (8, M), 0)

    second = []
    for j in range(CHUNKS + 1):
        if j == CAP:
            arrive(from_above)
        else:
            arrive(first[j])
        if j == CHUNKS - 1:
            arrive(from_below)
        low, high = rows_at(A_ENDS, j, 1)
        step(fu, low, high, 5, store_to(fv), first=True)
        zero_sides(fv, low, high)
        zero_rows(fv, low, high)
        low, high = rows_at(A_ENDS, j, 2)
        step(fv, low, high, 5, store_to(fu2))
        zero_sides(fu2, low, high)
        zero_rows(fu2, low, high)
        low, high = rows_at(A_ENDS, j, 3)
        step(fu2, low, high, 4, store_to(f3))
        items = [halo(t3, (low, high), edge_cols(dc, 0, 3), 0, dc) for dc in (-1, 1)]
        start(items)
        second.append(items)
        if j == CHUNKS - 1:
            again_from_above = again_from_row_neighbour(1)
            start(again_from_above)
        if j == CAP:
            again_from_below = again_from_row_neighbour(-1)
            start(again_from_below)
        if j in (0, 2):
            chain_stage(1 + j // 2)
    finish(first_sends)


    def store_end(row, base, new, first_row):
        for k, value in enumerate(new):
            end[row, 8 * k : 8 * k + 8, :] = value
        total = (new[0] + new[1]) + (new[2] + new[3])
        tot[pl.ds(row - DY if first_row >= DY else row + NY - DY, 1), :] = jnp.sum(total, axis=0, keepdims=True)

    def running(i, _):
        carry = jnp.zeros((1, M), jnp.float32)
        for k in range(4):
            value = end[i, 8 * k : 8 * k + 8, :]
            for shift in (1, 2, 4):
                value = value + jnp.where(place >= shift, pltpu.roll(value, shift, 0), 0.0)
            value = value + carry
            here[i, 8 * k : 8 * k + 8, :] = value
            carry = value[7:8, :]
        return 0

    def quarter(j):
        return pl.ds(j * QUARTER, QUARTER)

    def group_sum(j):
        arrive(totals[j])
        own = [p1[k, quarter(j), :] for k in range(4)]
        group[quarter(j), :] = (own[0] + own[1]) + (own[2] + own[3])
        items = [
            (g + k < 8, g >= k, copy_to(group.at[quarter(j), :], p2.at[g, quarter(j), :], {"rows": r, "cols": c + 4 * k}))
            for k in range(1, 8)
        ]
        start(items)
        return items

    totals, groups = [], []
    for j in range(CHUNKS + 1):
        arrive(second[j])
        if j == CHUNKS - 1:
            arrive(again_from_below)
        if j == CAP:
            arrive(again_from_above)
        low, high = rows_at(B_ENDS, j, 4)
        step(f3, low, high, 5, store_to(fv))
        zero_sides(fv, low, high)
        zero_rows(fv, low, high)
        low, high = rows_at(B_ENDS, j, 5)
        step(fv, low, high, 5, store_to(fu))
        zero_sides(fu, low, high)
        zero_rows(fu, low, high)
        low, high = rows_at(B_ENDS, j, 6)
        step(fu, low, high, 4, functools.partial(store_end, first_row=low), last=True)
        if j == CHUNKS - 1:
            continue
        k = min(j, CHUNKS - 1)
        items = [(None, None, copy_to(tot.at[quarter(k), :], p1.at[x, quarter(k), :], peer)) for peer in group_peers]
        start(items)
        totals.append(items)
        p1[x, quarter(k), :] = tot[quarter(k), :]
    chain_stage(3)
    for j in range(CHUNKS):
        groups.append(group_sum(j))
    lax.fori_loop(0, NY, running, 0, unroll=2)
    for j in range(CHUNKS):
        arrive(groups[j])
        before = jnp.zeros((QUARTER, M), jnp.float32)
        for k in range(7):
            before = before + jnp.where(k < g, p2[k, quarter(j), :], 0.0)
        for k in range(3):
            before = before + jnp.where(k < x, p1[k, quarter(j), :], 0.0)
        at = DY + j * QUARTER
        if j < CHUNKS - 1:
            below[at : at + QUARTER, :] = before
        else:
            below[at:NY, :] = before[: NY - at]
            below[0:DY, :] = before[NY - at :]
    finish()

PIECES = 4


def write_out(here, below, end, potential_out, end_out, potential, sems):
    rest = pltpu.make_async_copy(end, end_out, sems.at[PIECES])
    rest.start()
    rows = NY // PIECES
    pieces = []
    for k in range(PIECES):
        part = slice(k * rows, (k + 1) * rows)

        def row(i, _):
            potential[i] = (here[i] + below[pl.ds(i, 1), :]) * (1.0 / 1024)
            return 0

        lax.fori_loop(k * rows, (k + 1) * rows, row, 0, unroll=4)
        piece = pltpu.make_async_copy(potential.at[part], potential_out.at[part], sems.at[k])
        piece.start()
        pieces.append(piece)
    for piece in pieces:
        piece.wait()
    rest.wait()


def body(tracer, crowding):
    vmem = pl.BlockSpec(memory_space=pltpu.VMEM)
    hbm = pl.BlockSpec(memory_space=pltpu.HBM)
    f32 = jnp.float32
    dma = pltpu.SemaphoreType.DMA
    end, here, below = pl.pallas_call(
        kernel,
        out_shape=(
            jax.ShapeDtypeStruct((NY, NX, M), f32),
            jax.ShapeDtypeStruct((NY, NX, M), f32),
            jax.ShapeDtypeStruct((NY + 8, M), f32),
        ),
        in_specs=[hbm, hbm],
        out_specs=(vmem, vmem, vmem),
        scratch_shapes=[
            pltpu.VMEM((ROWS, PITCH, M), f32),
            pltpu.VMEM((ROWS, PITCH, M), f32),
            pltpu.VMEM((ROWS, PITCH, M), f32),
            pltpu.VMEM((ROWS, PITCH, M), f32),
            pltpu.VMEM((ROWS, PITCH, M), f32),
            pltpu.VMEM((NY + 8, M), f32),
            pltpu.VMEM((4, NY, M), f32),
            pltpu.VMEM((8, NY, M), f32),
            pltpu.VMEM((NY, M), f32),
            dma((2,)), dma((COUNT,)), dma((COUNT,)),
            pltpu.SemaphoreType.REGULAR((3,)),
        ],
        compiler_params=pltpu.CompilerParams(
            collective_id=0, has_side_effects=True, vmem_limit_bytes=50 * 1024 * 1024
        ),
    )(tracer, crowding)
    potential, end = pl.pallas_call(
        write_out,
        out_shape=(jax.ShapeDtypeStruct((NY, NX, M), f32), jax.ShapeDtypeStruct((NY, NX, M), f32)),
        in_specs=[vmem, vmem, vmem],
        out_specs=(hbm, hbm),
        scratch_shapes=[pltpu.VMEM((NY, NX, M), f32), dma((PIECES + 1,))],
        compiler_params=pltpu.CompilerParams(vmem_limit_bytes=8 * 1024 * 1024),
    )(here, below, end)
    return (potential, end)


def solution(mesh):
    spec = P("rows", "cols", None)
    return jax.shard_map(body, mesh=mesh, in_specs=(spec, spec), out_specs=(spec, spec), check_vma=False)
```
